512 devices in a mesh: gx: 8 (over x, core), gy: 8 (over z_lo), gz: 8 (over z_hi, y).
Axes of the slice: x: 4, y: 4, z: 16 (z_hi: 2, z_lo: 8; z = z_hi * 8 + z_lo), core: 2. Of those that a mesh axis runs over, the one named last changes fastest.
Arguments:
- volume: bfloat16 [4, 32, 64, 1024], P(None, 'gx', 'gy', 'gz'), may hold values from -6 to 6
- act_one: bfloat16 [16, 32, 64, 1024], P(None, 'gx', 'gy', 'gz'), may hold values from -6 to 6
- act_two: bfloat16 [16, 32, 64, 1024], P(None, 'gx', 'gy', 'gz'), may hold values from -6 to 6
- weight_one: bfloat16 [16, 4, 3, 3, 3], replicated, may hold values from -0.625 to 0.625
- weight_two: bfloat16 [16, 16, 3, 3, 3], replicated, may hold values from -0.3125 to 0.3125
- cotangent: bfloat16 [16, 32, 64, 1024], P(None, 'gx', 'gy', 'gz'), may hold values from -18 to 18
Outputs:
- grad_weight_one: float32 [16, 4, 3, 3, 3], replicated
- grad_bias_one: float32 [16], replicated
- grad_weight_two: float32 [16, 16, 3, 3, 3], replicated
- grad_bias_two: float32 [16], replicated
- grad_volume: float32 [4, 32, 64, 1024], P(None, 'gx', 'gy', 'gz')
The draws below stay inside these ranges and needn't reach their ends.
All inputs are finite; a program needn't handle non-finite values.
Results may differ from the reference program's by a relative error of at most 0.0055.
Values may be sent and summed in bfloat16 or wider, within the bound.
A program may use at most 64 MiB of HBM per device.

```python
import math
import jax
import jax.numpy as jnp
from jax import lax

CHAN_IN = 4
CHAN = 16
NX = 32
NY = 64
NZ = 1024


def draw_cotangent(key, part):
    extent = (CHAN, NX, NY, NZ)
    rising = 1.0 + 2.0 * jnp.arange(NX, dtype=jnp.float32) / (NX - 1)
    values = jax.random.normal(key, extent, jnp.float32)
    return jnp.clip(values * rising[None, :, None, None], -18.0, 18.0).astype(jnp.bfloat16)


def block_scale(own_key, dims, shards, least, top_value):
    def one(axis_at, blocks):
        heights = jax.random.uniform(jax.random.fold_in(jax.random.fold_in(own_key, 6), axis_at), (blocks,), jnp.float32, least / len(shards), top_value / len(shards))
        return jnp.repeat(jnp.exp(heights), dims[axis_at] // blocks).reshape((-1,) + (1,) * (len(dims) - axis_at - 1))

    level = one(*shards[0])
    for cut in shards[1:]:
        level = level * one(*cut)
    return level


def normal_values(own_key, shape, spread, limit, cuts=(), kind=jnp.bfloat16):
    factor_of = block_scale(own_key, shape, cuts, -0.22, 0.18) if cuts else 1.0
    array = jax.random.normal(own_key, shape, jnp.float32) * spread * factor_of
    return jnp.minimum(jnp.maximum(array, -limit), limit).astype(kind)


def setup_inputs(seed: int = 0) -> dict:
    arg_keys = jax.random.split(jax.random.key(seed), 7)
    return {
        "volume": normal_values(arg_keys[0], (CHAN_IN, NX, NY, NZ), 1.0, 6.0, ((1, 8), (2, 8), (3, 8))),
        "act_one": normal_values(arg_keys[1], (CHAN, NX, NY, NZ), 1.0, 6.0, ((1, 8), (2, 8), (3, 8))),
        "act_two": normal_values(arg_keys[2], (CHAN, NX, NY, NZ), 1.0, 6.0, ((1, 8), (2, 8), (3, 8))),
        "weight_one": normal_values(arg_keys[3], (CHAN, CHAN_IN, 3, 3, 3), (CHAN_IN * 27) ** -0.5, 0.625),
        "weight_two": normal_values(arg_keys[4], (CHAN, CHAN, 3, 3, 3), (CHAN * 27) ** -0.5, 0.3125),
        "cotangent": draw_cotangent(jax.random.fold_in(arg_keys[6], 71), 0),
    }


def slope_of(saved):
    return jnp.where(saved > 0, 1.0, 0.3).astype(jnp.float32)

def tap_list():
    return [(tap_x, tap_y, tap_z) for tap_x in range(3) for tap_y in range(3) for tap_z in range(3)]

def weight_grad(delta, source):
    outputs = delta.shape[0]
    inputs = source.shape[0]
    flat_delta = delta.reshape(outputs, -1)
    columns = []
    for tap_x, tap_y, tap_z in tap_list():
        shifted = jnp.roll(source, (1 - tap_x, 1 - tap_y, 1 - tap_z), axis=(1, 2, 3))
        columns.append(jnp.dot(flat_delta, shifted.reshape(inputs, -1).T, preferred_element_type=jnp.float32))
    return jnp.stack(columns, -1).reshape(outputs, inputs, 3, 3, 3)

def back_through(weights, delta):
    outputs = delta.shape[0]
    inputs = weights.shape[1]
    total = jnp.zeros((inputs, delta.shape[1] * delta.shape[2] * delta.shape[3]), jnp.float32)
    for tap_x, tap_y, tap_z in tap_list():
        shifted = jnp.roll(delta, (tap_x - 1, tap_y - 1, tap_z - 1), axis=(1, 2, 3))
        total = total + jnp.dot(weights[:, :, tap_x, tap_y, tap_z].T, shifted.reshape(outputs, -1), preferred_element_type=jnp.float32)
    return total.reshape((inputs,) + delta.shape[1:])

def reference(volume, act_one, act_two, weight_one, weight_two, cotangent):
    norm = 1.0 / math.sqrt(NX * NY * NZ)
    delta_two = (cotangent.astype(jnp.float32) * slope_of(act_two)).astype(jnp.bfloat16)
    grad_bias_two = lax.optimization_barrier(jnp.sum(delta_two.astype(jnp.float32), axis=(1, 2, 3))) * norm
    grad_weight_two = weight_grad(delta_two, act_one) * norm
    back = back_through(weight_two, delta_two)
    delta_one = (back * slope_of(act_one)).astype(jnp.bfloat16)
    grad_bias_one = lax.optimization_barrier(jnp.sum(delta_one.astype(jnp.float32), axis=(1, 2, 3))) * norm
    grad_weight_one = weight_grad(delta_one, volume) * norm
    grad_volume = back_through(weight_one, delta_one)
    return (grad_weight_one, grad_bias_one, grad_weight_two, grad_bias_two, grad_volume)
```

```python
import functools
import math

import jax
import jax.numpy as jnp
import numpy as np
from jax import lax
from jax.experimental import pallas as pl
from jax.experimental.pallas import tpu as pltpu
from jax.sharding import PartitionSpec as P

CHAN_IN = 4
CHAN = 16
NX, NY, NZ = 4, 8, 128
F32, BF16 = jnp.float32, jnp.bfloat16
MESH = pl.DeviceIdType.MESH
ROWS = 3
SIDES = ((-1, 0), (1, 0), (0, -1), (0, 1), (-1, -1), (-1, 1), (1, -1), (1, 1))


def constants():
    r = np.arange(128)
    perm = np.zeros((128, 128), np.float32)
    perm[r, (r % 16) * 8 + r // 16] = 1
    eye = np.eye(128, dtype=np.float32)
    ends = np.zeros((16, 128), np.float32)
    ends[0, 0] = ends[1, 127] = 1
    tiles = np.zeros((32, 128), np.float32)
    for h in range(2):
        for x in range(4):
            for j in range(4):
                tiles[h * 16 + x * 4 + j, j * 32 + x * 8 + 7 * h] = 1
    rim_cols = np.zeros((48, 128), np.float32)
    rim_rows = np.zeros((48, 128), np.float32)
    for p in range(6):
        x = (p - 1) % 4
        for h in range(2):
            for j in range(4):
                rim_cols[p * 8 + h * 4 + j, j * 32 + x * 8 + 7 * (1 - h)] = 1
                tile = h if 1 <= p <= 4 else 2 + (0 if p == 0 else 2) + h
                rim_rows[p * 8 + h * 4 + j, tile * 16 + x * 4 + j] = 1
    spread = np.zeros((128, 128), np.float32)
    spread[r, r % 16] = 1
    narrow = np.concatenate([perm, eye, ends, tiles, rim_cols, rim_rows, spread])
    lane = np.arange(512)
    inside = lane < 480
    tap, end, chan = lane // 160, (lane % 160) // 16, lane % 16
    place = np.zeros((48, 512), np.float32)
    for c in range(3):
        for o in range(16):
            place[c * 16 + o] = inside & (tap == c) & (chan == o)
    y_two = (np.arange(128) // 16)[:, None]
    y_one = (np.arange(32) % 8)[:, None]
    band_two = np.where(inside[None], y_two + 2 - end[None], -9)
    band_one = np.where(inside[None], y_one + 2 - end[None], -9)
    wide = np.concatenate([place, band_two, band_one])
    rr = np.arange(128) % 40
    ok = np.arange(128) < 120
    row_y = np.where(rr < 32, 1 + rr % 8, np.where(rr < 36, 0, 9))
    row_j = np.where(rr < 32, rr // 8, rr % 4)
    row_c = np.arange(128) // 40
    y_of = np.broadcast_to(np.where(ok, row_y, -9)[None], (16, 128))
    fold = np.zeros((9, 128, 128), np.float32)
    for ab in range(9):
        for q in range(120):
            fold[ab, q, (ab * 3 + row_c[q]) * 4 + row_j[q]] = 1
    narrow = np.concatenate([narrow, y_of, fold.reshape(-1, 128)])
    return jnp.asarray(narrow, BF16), jnp.asarray(wide, BF16)


AT = {}
_at = 0
for _name, _n in (("perm", 128), ("eye", 128), ("ends", 16), ("tiles", 32), ("rim_cols", 48), ("rim_rows", 48), ("spread", 128), ("y_of", 16), ("fold", 1152)):
    AT[_name] = (_at, _n)
    _at += _n
NARROW = _at


def nt(a, b):
    return lax.dot_general(a, b, (((1,), (1,)), ((), ())), preferred_element_type=F32)


def nn(a, b):
    return jnp.dot(a, b, preferred_element_type=F32)


def way(dx, dy):
    return (dx + 1) * 3 + dy + 1


def corner(dx, dy):
    return (dx + 1) + (dy + 1) // 2


def kernel(
    sizes, norm,
    vol_h, act1_h, act2_h, w1_h, w2_h, cot_h, narrow_h, wide_h,
    gw1, gb1, gw2, gb2, gvol,
    vol_v, act1_v, act2_v, w1_v, w2_v, cot_v, narrow_v, wide_v,
    xs, xr, ys, yr, xyr, zs, zr,
    xs2, xr2, ys2, yr2, xyr2, zs2, zr2,
    inner, acts, planes, volp, m_two, m_one, share, got1, got2, mid1, mid2, summed,
    load_sem, own_sem, send_sem, recv_sem, red_send, red_recv,
):
    n_gx, n_gy, n_gz = sizes
    n_y = 4
    n_hi = n_gz // n_y
    n_group = n_gx * n_y
    n_line = n_gy * n_hi
    gx, gy, gz = lax.axis_index("gx"), lax.axis_index("gy"), lax.axis_index("gz")
    y_pos, hi_pos = lax.rem(gz, n_y), lax.div(gz, n_y)
    group_at = gx * n_y + y_pos
    line_at = hi_pos * n_gy + gy

    def near(dx, dy, dz):
        return (
            lax.rem(gx + (n_gx + dx), n_gx),
            lax.rem(gy + (n_gy + dy), n_gy),
            lax.rem(gz + (n_gz + dz), n_gz),
        )

    def in_group(k):
        t = lax.rem(group_at + k, n_group)
        return t, (lax.div(t, n_y), gy, hi_pos * n_y + lax.rem(t, n_y))

    def in_line(k):
        t = lax.rem(line_at + k, n_line)
        return t, (gx, lax.rem(t, n_gy), lax.div(t, n_gy) * n_y + y_pos)

    barrier = pltpu.get_barrier_semaphore()
    for dz in (-1, 1, 0):
        for dx in (-1, 0, 1):
            for dy in (-1, 0, 1):
                if (dx, dy, dz) != (0, 0, 0):
                    pl.semaphore_signal(barrier, inc=1, device_id=near(dx, dy, dz), device_id_type=MESH)

    def greet_line(k, _):
        pl.semaphore_signal(barrier, inc=1, device_id=in_line(k)[1], device_id_type=MESH)
        return 0

    def greet_group(k, _):
        pl.semaphore_signal(barrier, inc=1, device_id=in_group(k)[1], device_id_type=MESH)
        return 0

    lax.fori_loop(1, n_line, greet_line, 0)
    lax.fori_loop(1, n_group, greet_group, 0)

    loads = [
        pltpu.make_async_copy(src, dst, load_sem.at[i])
        for i, (src, dst) in enumerate(
            ((cot_h, cot_v), (act2_h, act2_v), (narrow_h, narrow_v), (vol_h, vol_v), (act1_h, act1_v), (wide_h, wide_v), (w2_h, w2_v), (w1_h, w1_v))
        )
    ]
    for copy in loads:
        copy.start()

    def const(name):
        at, n = AT[name]
        return narrow_v[at : at + n, :]

    for i in range(4):
        loads[i].wait()
    perm, eye, ends = const("perm"), const("eye"), const("ends")

    def rows_of(ref, x):
        return ref[:, x].astype(F32).reshape(128, 128)

    def edge_rows(inner_at):
        return jnp.concatenate(
            [inner_at(x)[0:16] for x in range(4)] + [inner_at(x)[112:128] for x in range(4)], axis=0
        )

    row8 = lax.broadcasted_iota(jnp.int32, (8, 128), 0)

    def stack8(rows):
        out = jnp.zeros((8, 128), F32)
        for i, row in enumerate(rows):
            out = jnp.where(row8 == i, jnp.broadcast_to(row, (8, 128)), out)
        return out

    deltas = []
    for x in range(4):
        v = rows_of(cot_v, x)
        deltas.append(jnp.where(rows_of(act2_v, x) > 0, v, v * 0.3).astype(BF16))
    turned = nn(perm, jnp.concatenate(deltas, axis=1))
    bias_two = turned[:, 0:128] + turned[:, 128:256] + turned[:, 256:384] + turned[:, 384:512]
    turned = turned.astype(BF16)
    for x in range(4):
        inner[x] = turned[:, x * 128 : (x + 1) * 128]
    volflat = vol_v[...].astype(F32).reshape(128, 128).astype(BF16)
    vol_tiles = nn(const("tiles"), volflat).astype(BF16)

    def vol_rows(x):
        return vol_v[:, x].astype(F32).reshape(32, 128)

    xs[0, 0:128] = inner[0]
    xs[1, 0:128] = inner[3]
    xs[0, 128:160] = vol_rows(0).astype(BF16)
    xs[1, 128:160] = vol_rows(3).astype(BF16)
    for h in range(2):
        for at, x in ((0, 0), (2, 3), (3, 1), (4, 2)):
            ys[h, at * 16 : at * 16 + 16] = inner[x][112 * h : 112 * h + 16]
        ys[h, 16:32] = vol_tiles[16 * h : 16 * h + 16]
    z_face = nt(ends, jnp.concatenate([inner[x] for x in range(4)], axis=0))
    z_edge = nt(ends, edge_rows(lambda x: inner[x]))
    z_vol = nt(ends, volflat)
    for f in range(2):
        face = [z_face[f : f + 1, x * 128 : (x + 1) * 128] for x in range(4)]
        edge, flat = z_edge[f : f + 1], z_vol[f : f + 1]
        zs[f] = stack8([face[1], face[2], face[0], flat, face[3], edge, flat])

    pl.semaphore_wait(barrier, 26 + (n_line - 1) + (n_group - 1))

    def exchange(phase, xs, xr, ys, yr, xyr, zs, zr):
        first = phase == 0
        out = []

        def send(kind, src, dst, where):
            copy = pltpu.make_async_remote_copy(
                src, dst, send_sem.at[phase, kind], recv_sem.at[phase, kind], device_id=where, device_id_type=MESH
            )
            copy.start()
            out.append(copy)

        for dz in (-1, 1):
            f, side = (1 if dz == 1 else 0), (0 if dz == 1 else 1)
            for dx in (-1, 0, 1):
                for dy in (-1, 0, 1):
                    if first:
                        at, n = {-1: (2, 2), 1: (3, 2), 0: (0, 5) if dy == 0 else (5, 2)}[dx]
                    else:
                        at, n = {-1: (2, 1), 1: (3, 1), 0: (0, 4) if dy == 0 else (4, 1)}[dx]
                    send(0, zs.at[f, pl.ds(at, n)], zr.at[side, pl.ds(8 * way(-dx, -dy), n)], near(dx, dy, dz))
        for dx in (-1, 1):
            send(1, xs.at[(dx + 1) // 2], xr.at[(1 - dx) // 2], near(dx, 0, 0))
        for dy in (-1, 1):
            send(2, ys.at[(dy + 1) // 2], yr.at[(1 - dy) // 2], near(0, dy, 0))
        for dx in (-1, 1):
            for dy in (-1, 1):
                if first:
                    at, n = (0 if dx == -1 else 16), 32
                else:
                    at, n = (0 if dx == -1 else 16), 16
                send(3, ys.at[(dy + 1) // 2, pl.ds(at, n)], xyr.at[corner(-dx, -dy)], near(dx, dy, 0))

    def settle(sems, phase, xr, yr, xyr, zr):
        n = 42 if phase == 0 else 24
        for kind, ref in ((0, zr.at[0, pl.ds(0, n)]), (1, xr), (2, yr), (3, xyr)):
            pltpu.make_async_copy(ref, ref, sems.at[phase, kind]).wait()

    lane_of = lax.broadcasted_iota(jnp.int32, (160, 128), 1)

    def build_planes(phase, inner_at, xr, yr, xyr, zr):
        first = phase == 0
        cols = nt(eye, zr[...].reshape(144, 128).astype(BF16))
        tile_at = {0: 0, 3: 2, 1: 3, 2: 4} if first else {0: 0, 3: 1, 1: 2, 2: 3}
        face_at = {0: 2, 3: 4, 1: 0, 2: 1} if first else {0: 2, 3: 3, 1: 0, 2: 1}
        for p in range(6):
            if 1 <= p <= 4:
                x = p - 1
                low = yr[0, tile_at[x] * 16 : tile_at[x] * 16 + 16]
                mid = inner_at(x)
                high = yr[1, tile_at[x] * 16 : tile_at[x] * 16 + 16]
                pick = (
                    (64 + 16 * x, 80 + 16 * x, 8 * way(0, -1)),
                    (0, 128, 8 * way(0, 0) + face_at[x]),
                    (16 * x, 16 * x + 16, 8 * way(0, 1)),
                )
            else:
                dx = -1 if p == 0 else 1
                at = (16 if dx == -1 else 0) if first else 0
                low = xyr[corner(dx, -1), at : at + 16]
                mid = xr[(dx + 1) // 2, 0:128]
                high = xyr[corner(dx, 1), at : at + 16]
                r = (1 if dx == -1 else 0) if first else 0
                pick = (
                    (112, 128, 8 * way(dx, -1) + r),
                    (0, 128, 8 * way(dx, 0) + r),
                    (0, 16, 8 * way(dx, 1) + r),
                )
            plane = jnp.concatenate([low, mid, high], axis=0)
            lanes = slice(p * 128, (p + 1) * 128)
            planes[160:320, lanes] = plane
            plane = plane.astype(F32)
            for tap, side, turn, lane in ((0, 1, 127, 127), (2, 0, 1, 0)):
                col = jnp.concatenate(
                    [cols[a:b, 72 * side + k : 72 * side + k + 1] for a, b, k in pick], axis=0
                )
                shifted = jnp.where(lane_of == lane, jnp.broadcast_to(col, (160, 128)), pltpu.roll(plane, turn, 1))
                planes[tap * 160 : tap * 160 + 160, lanes] = shifted.astype(BF16)
        return cols

    exchange(0, xs, xr, ys, yr, xyr, zs, zr)

    for i in range(4, 8):
        loads[i].wait()
    turned = nn(perm, jnp.concatenate([rows_of(act1_v, x).astype(BF16) for x in range(4)], axis=1))
    acts[...] = turned.astype(BF16)
    planes[480:512, :] = jnp.zeros((32, 768), BF16)
    place = wide_v[0:48, :]
    band_two = wide_v[48:176, :].astype(F32)
    band_one = wide_v[176:208, :].astype(F32)
    spread = const("spread")[:, 0:16]
    for a in range(3):
        total_two = jnp.zeros((128, 512), F32)
        total_one = jnp.zeros((32, 512), F32)
        for b in range(3):
            t = (a * 3 + b) * 3
            group = w2_v[t : t + 3].reshape(48, 16)
            wide = nn(nt(spread, group).astype(BF16), place)
            total_two = jnp.where(band_two == b, wide, total_two)
            four = jnp.zeros((4, 512), F32)
            for c in range(3):
                four = four + nn(w1_v[t + c], place[c * 16 : c * 16 + 16])
            wide = jnp.concatenate([jnp.broadcast_to(four[j : j + 1], (8, 512)) for j in range(4)], axis=0)
            total_one = jnp.where(band_one == b, wide, total_one)
        m_two[a] = total_two.astype(BF16)
        m_one[a] = total_one.astype(BF16)

    settle(recv_sem, 0, xr, yr, xyr, zr)
    cols = build_planes(0, lambda x: inner[x], xr, yr, xyr, zr)

    back = nn(m_two[0], planes[:, 256:768]) + nn(m_two[1], planes[:, 128:640]) + nn(m_two[2], planes[:, 0:512])
    delta = jnp.where(acts[...].astype(F32) > 0, back, back * 0.3).astype(BF16)
    wide_delta = delta.astype(F32)
    bias_one = wide_delta[:, 0:128] + wide_delta[:, 128:256] + wide_delta[:, 256:384] + wide_delta[:, 384:512]

    def delta_at(x):
        return delta[:, x * 128 : (x + 1) * 128]

    xs2[0] = delta_at(0)
    xs2[1] = delta_at(3)
    for h in range(2):
        for at, x in ((0, 0), (1, 3), (2, 1), (3, 2)):
            ys2[h, at * 16 : at * 16 + 16] = delta_at(x)[112 * h : 112 * h + 16]
    z_face = nt(ends, jnp.concatenate([delta_at(x) for x in range(4)], axis=0))
    z_edge = nt(ends, edge_rows(delta_at))
    for f in range(2):
        face = [z_face[f : f + 1, x * 128 : (x + 1) * 128] for x in range(4)]
        zs2[f] = stack8([face[1], face[2], face[0], face[3], z_edge[f : f + 1]])
    exchange(1, xs2, xr2, ys2, yr2, xyr2, zs2, zr2)
    for x in range(4):
        inner[x] = delta_at(x)

    v_tiles = jnp.concatenate(
        [yr[0, 16:32], yr[1, 16:32]]
        + [xyr[corner(dx, dy), at : at + 16] for dx, at in ((-1, 0), (1, 16)) for dy in (-1, 1)],
        axis=0,
    )
    rims = nn(const("rim_rows")[:, 0:96], v_tiles)
    rim_cols = nn(const("rim_cols"), cols.astype(BF16))
    lane40 = lax.broadcasted_iota(jnp.int32, (40, 128), 1)
    half8 = lax.broadcasted_iota(jnp.int32, (8, 1), 0) < 4
    volp[120:128, :] = jnp.zeros((8, 768), F32)
    for p in range(6):
        x = (p - 1) % 4
        dx = -1 if p == 0 else (1 if p == 5 else 0)
        mid = vol_rows(x) if dx == 0 else xr[(dx + 1) // 2, 128:160].astype(F32)
        plane = jnp.concatenate([mid, rims[p * 8 : p * 8 + 8]], axis=0)
        lanes = slice(p * 128, (p + 1) * 128)
        volp[40:80, lanes] = plane
        r = {-1: 0, 1: 1, 0: 1}[dx]
        for tap, side, turn, lane in ((0, 0, 1, 0), (2, 1, 127, 127)):
            k = 72 * side + 8 * way(dx, 0) + (3 if dx == 0 else r)
            col = jnp.concatenate(
                [cols[j * 32 + x * 8 : j * 32 + x * 8 + 8, k : k + 1] for j in range(4)]
                + [
                    jnp.where(
                        half8,
                        rim_cols[p * 8 : p * 8 + 8, 72 * side + 8 * way(dx, -1) + r : 72 * side + 8 * way(dx, -1) + r + 1],
                        rim_cols[p * 8 : p * 8 + 8, 72 * side + 8 * way(dx, 1) + r : 72 * side + 8 * way(dx, 1) + r + 1],
                    )
                ],
                axis=0,
            )
            volp[tap * 40 : tap * 40 + 40, lanes] = jnp.where(
                lane40 == lane, jnp.broadcast_to(col, (40, 128)), pltpu.roll(plane, turn, 1)
            )

    y_of = const("y_of").astype(F32)
    sums = []
    for a in range(3):
        g = nt(delta, volp[:, a * 128 : (a + 4) * 128].astype(BF16))
        for b in range(3):
            total = jnp.zeros((16, 128), F32)
            for y in range(8):
                total = total + jnp.where(y_of == y + b, g[y * 16 : y * 16 + 16], 0.0)
            sums.append(total)
    sums = jnp.concatenate(sums, axis=1)
    top = sums.astype(BF16)
    rest = (sums - top.astype(F32)).astype(BF16)
    fold = const("fold")
    packed = nn(top, fold) + nn(rest, fold)

    def fold_y(v):
        out = v[0:16]
        for y in range(1, 8):
            out = out + v[y * 16 : y * 16 + 16]
        return jnp.broadcast_to(jnp.sum(out, axis=1, keepdims=True), (16, 128))

    lane16 = lax.broadcasted_iota(jnp.int32, (16, 128), 1)
    share[64:80] = jnp.where(lane16 >= 108, fold_y(bias_one), packed)
    share[80:96] = jnp.zeros((16, 128), F32)

    slot = lax.shift_right_logical(lane16, 4)
    blocks = [jnp.zeros((16, 128), F32) for _ in range(4)]
    for a in range(3):
        g = nt(planes[0:480, (2 - a) * 128 : (6 - a) * 128], acts[...])
        for b in range(3):
            for c in range(3):
                t = (a * 3 + b) * 3 + c
                total = jnp.zeros((16, 128), F32)
                for y in range(8):
                    at = c * 160 + (y + 2 - b) * 16
                    total = jnp.where(slot == y, g[at : at + 16], total)
                for turn in (64, 32, 16):
                    total = total + pltpu.roll(total, turn, 1)
                blocks[t // 8] = jnp.where(slot == t % 8, total, blocks[t // 8])
    blocks[3] = jnp.where(slot == 3, fold_y(bias_two), blocks[3])
    for k in range(4):
        share[k * 16 : k * 16 + 16] = blocks[k]

    def scatter(k, _):
        t, where = in_group(k)
        pltpu.make_async_remote_copy(
            share.at[pl.ds(ROWS * t, ROWS)], got1.at[pl.ds(4 * group_at, ROWS)],
            red_send.at[0], red_recv.at[0], device_id=where, device_id_type=MESH,
        ).start()
        return 0

    lax.fori_loop(1, n_group, scatter, 0)
    own = pltpu.make_async_copy(share.at[pl.ds(ROWS * group_at, ROWS)], got1.at[pl.ds(4 * group_at, ROWS)], own_sem.at[0])
    own.start()
    own.wait()

    def await_rows(sem, ref, n):
        ref = ref.at[pl.ds(0, n * ROWS)]
        pltpu.make_async_copy(ref, ref, sem).wait()

    def total8(ref, n):
        out = ref[0:8]
        for i in range(1, n // 2):
            out = out + ref[i * 8 : i * 8 + 8]
        return out + pltpu.roll(out, 4, 0)

    await_rows(red_recv.at[0], got1, n_group - 1)
    mid1[...] = total8(got1, n_group)

    def along(k, _):
        _, where = in_line(k)
        pltpu.make_async_remote_copy(
            mid1.at[pl.ds(0, ROWS)], got2.at[pl.ds(4 * line_at, ROWS)],
            red_send.at[1], red_recv.at[1], device_id=where, device_id_type=MESH,
        ).start()
        return 0

    lax.fori_loop(1, n_line, along, 0)
    own = pltpu.make_async_copy(mid1.at[pl.ds(0, ROWS)], got2.at[pl.ds(4 * line_at, ROWS)], own_sem.at[1])
    own.start()
    own.wait()

    settle(recv_sem, 1, xr2, yr2, xyr2, zr2)
    build_planes(1, lambda x: inner[x], xr2, yr2, xyr2, zr2)
    grad = nn(m_one[0], planes[:, 256:768]) + nn(m_one[1], planes[:, 128:640]) + nn(m_one[2], planes[:, 0:512])
    for j in range(4):
        for x in range(4):
            gvol[j, x] = grad[j * 8 : j * 8 + 8, x * 128 : (x + 1) * 128]

    await_rows(red_recv.at[1], got2, n_line - 1)
    mid2[...] = total8(got2, n_line) * norm

    def gather(k, _):
        _, where = in_group(k)
        pltpu.make_async_remote_copy(
            mid2.at[pl.ds(0, ROWS)], summed.at[pl.ds(ROWS * group_at, ROWS)],
            red_send.at[2], red_recv.at[2], device_id=where, device_id_type=MESH,
        ).start()
        return 0

    lax.fori_loop(1, n_group, gather, 0)
    own = pltpu.make_async_copy(mid2.at[pl.ds(0, ROWS)], summed.at[pl.ds(ROWS * group_at, ROWS)], own_sem.at[2])
    own.start()
    own.wait()
    settle(send_sem, 0, xr, yr, xyr, zr)
    settle(send_sem, 1, xr2, yr2, xyr2, zr2)
    await_rows(red_send.at[0], got1, n_group - 1)
    await_rows(red_send.at[1], got2, n_line - 1)
    await_rows(red_recv.at[2], summed, n_group - 1)

    for k in range(4):
        block = summed[k * 16 : k * 16 + 16]
        for s in range(8):
            if k * 8 + s < 27:
                turned = pltpu.roll(block, (128 - 16 * s) % 128, 1) if s else block
                gw2[k * 8 + s] = turned[:, 0:16]
    gb2[...] = summed[48:64].T[48:49, :]
    packed = summed[64:80].T
    for t in range(27):
        gw1[t] = packed[4 * t : 4 * t + 4, :]
    gb1[...] = packed[108:109, :]
    await_rows(red_send.at[2], summed, n_group - 1)


def local(sizes, norm, volume, act_one, act_two, weight_one, weight_two, cotangent):
    narrow, wide = constants()
    w1 = jnp.transpose(weight_one, (2, 3, 4, 1, 0)).reshape(27, CHAN_IN, CHAN)
    w2 = jnp.transpose(weight_two, (2, 3, 4, 0, 1)).reshape(27, CHAN, CHAN)
    n_group = sizes[0] * 4
    n_line = sizes[1] * (sizes[2] // 4)
    buf = lambda *shape: pltpu.VMEM(shape, BF16)
    buf32 = lambda *shape: pltpu.VMEM(shape, F32)
    block = (CHAN, NX, NY, NZ)
    gw1, gb1, gw2, gb2, gvol = pl.pallas_call(
        functools.partial(kernel, sizes, norm),
        out_shape=(
            jax.ShapeDtypeStruct((27, CHAN_IN, CHAN), F32),
            jax.ShapeDtypeStruct((1, CHAN), F32),
            jax.ShapeDtypeStruct((27, CHAN, CHAN), F32),
            jax.ShapeDtypeStruct((1, CHAN), F32),
            jax.ShapeDtypeStruct((CHAN_IN, NX, NY, NZ), F32),
        ),
        in_specs=[pl.BlockSpec(memory_space=pl.ANY)] * 8,
        out_specs=tuple([pl.BlockSpec(memory_space=pltpu.VMEM)] * 5),
        scratch_shapes=[
            buf(CHAN_IN, NX, NY, NZ), buf(*block), buf(*block), buf(27, CHAN_IN, CHAN), buf(27, CHAN, CHAN), buf(*block),
            buf(NARROW, 128), buf(208, 512),
            buf(2, 160, 128), buf(2, 160, 128), buf(2, 80, 128), buf(2, 80, 128), buf(4, 32, 128), buf32(2, 8, 128), buf32(2, 72, 128),
            buf(2, 128, 128), buf(2, 128, 128), buf(2, 64, 128), buf(2, 64, 128), buf(4, 16, 128), buf32(2, 8, 128), buf32(2, 72, 128),
            buf(4, 128, 128), buf(128, 512), buf(512, 768), buf32(128, 768), buf(3, 128, 512), buf(3, 32, 512),
            buf32(96, 128), buf32(4 * n_group, 128), buf32(4 * n_line, 128), buf32(8, 128), buf32(8, 128), buf32(96, 128),
            pltpu.SemaphoreType.DMA((8,)), pltpu.SemaphoreType.DMA((3,)),
            pltpu.SemaphoreType.DMA((2, 4)), pltpu.SemaphoreType.DMA((2, 4)),
            pltpu.SemaphoreType.DMA((3,)), pltpu.SemaphoreType.DMA((3,)),
        ],
        compiler_params=pltpu.CompilerParams(collective_id=0, has_side_effects=True),
        name="both_layers",
    )(volume, act_one, act_two, w1, w2, cotangent, narrow, wide)
    gw1 = jnp.transpose(gw1.reshape(3, 3, 3, CHAN_IN, CHAN), (4, 3, 0, 1, 2))
    gw2 = jnp.transpose(gw2.reshape(3, 3, 3, CHAN, CHAN), (3, 4, 0, 1, 2))
    return gw1, gb1.reshape(CHAN), gw2, gb2.reshape(CHAN), gvol


def solution(mesh):
    sizes = tuple(mesh.shape[name] for name in ("gx", "gy", "gz"))
    norm = 1.0 / math.sqrt(NX * NY * NZ * sizes[0] * sizes[1] * sizes[2])
    block = P(None, "gx", "gy", "gz")
    return jax.shard_map(
        functools.partial(local, sizes, norm),
        mesh=mesh,
        in_specs=(block, block, block, P(), P(), block),
        out_specs=(P(), P(), P(), P(), block),
        check_vma=False,
    )
```

```python
import functools
import math

import jax
import jax.numpy as jnp
import numpy as np
from jax import lax
from jax.experimental import pallas as pl
from jax.experimental.pallas import tpu as pltpu
from jax.sharding import PartitionSpec as P

CHAN_IN = 4
CHAN = 16
NX, NY, NZ = 4, 8, 128
F32, BF16 = jnp.float32, jnp.bfloat16
MESH = pl.DeviceIdType.MESH
ROWS = 3
SIDES = ((-1, 0), (1, 0), (0, -1), (0, 1), (-1, -1), (-1, 1), (1, -1), (1, 1))


def constants():
    r = np.arange(128)
    perm = np.zeros((128, 128), np.float32)
    perm[r, (r % 16) * 8 + r // 16] = 1
    eye = np.eye(128, dtype=np.float32)
    ends = np.zeros((16, 128), np.float32)
    ends[0, 0] = ends[1, 127] = 1
    tiles = np.zeros((32, 128), np.float32)
    for h in range(2):
        for x in range(4):
            for j in range(4):
                tiles[h * 16 + x * 4 + j, j * 32 + x * 8 + 7 * h] = 1
    rim_cols = np.zeros((48, 128), np.float32)
    rim_rows = np.zeros((48, 128), np.float32)
    for p in range(6):
        x = (p - 1) % 4
        for h in range(2):
            for j in range(4):
                rim_cols[p * 8 + h * 4 + j, j * 32 + x * 8 + 7 * (1 - h)] = 1
                tile = h if 1 <= p <= 4 else 2 + (0 if p == 0 else 2) + h
                rim_rows[p * 8 + h * 4 + j, tile * 16 + x * 4 + j] = 1
    spread = np.zeros((128, 128), np.float32)
    spread[r, r % 16] = 1
    narrow = np.concatenate([perm, eye, ends, tiles, rim_cols, rim_rows, spread])
    lane = np.arange(512)
    inside = lane < 480
    tap, end, chan = lane // 160, (lane % 160) // 16, lane % 16
    place = np.zeros((48, 512), np.float32)
    for c in range(3):
        for o in range(16):
            place[c * 16 + o] = inside & (tap == c) & (chan == o)
    y_two = (np.arange(128) // 16)[:, None]
    y_one = (np.arange(32) % 8)[:, None]
    band_two = np.where(inside[None], y_two + 2 - end[None], -9)
    band_one = np.where(inside[None], y_one + 2 - end[None], -9)
    wide = np.concatenate([place, band_two, band_one])
    rr = np.arange(128) % 40
    ok = np.arange(128) < 120
    row_y = np.where(rr < 32, 1 + rr % 8, np.where(rr < 36, 0, 9))
    row_j = np.where(rr < 32, rr // 8, rr % 4)
    row_c = np.arange(128) // 40
    y_of = np.broadcast_to(np.where(ok, row_y, -9)[None], (16, 128))
    fold = np.zeros((9, 128, 128), np.float32)
    for ab in range(9):
        for q in range(120):
            fold[ab, q, (ab * 3 + row_c[q]) * 4 + row_j[q]] = 1
    narrow = np.concatenate([narrow, y_of, fold.reshape(-1, 128)])
    return jnp.asarray(narrow, BF16), jnp.asarray(wide, BF16)


AT = {}
_at = 0
for _name, _n in (("perm", 128), ("eye", 128), ("ends", 16), ("tiles", 32), ("rim_cols", 48), ("rim_rows", 48), ("spread", 128), ("y_of", 16), ("fold", 1152)):
    AT[_name] = (_at, _n)
    _at += _n
NARROW = _at


def nt(a, b):
    return lax.dot_general(a, b, (((1,), (1,)), ((), ())), preferred_element_type=F32)


def nn(a, b):
    return jnp.dot(a, b, preferred_element_type=F32)


def way(dx, dy):
    return (dx + 1) * 3 + dy + 1


def corner(dx, dy):
    return (dx + 1) + (dy + 1) // 2


def kernel(
    sizes, norm,
    vol_h, act1_h, act2_h, w1_h, w2_h, cot_h, narrow_h, wide_h,
    summed, gvol,
    vol_v, act1_v, act2_v, w1_v, w2_v, cot_v, narrow_v, wide_v,
    xs, xr, ys, yr, xyr, zs, zr,
    xs2, xr2, ys2, yr2, xyr2, zs2, zr2,
    inner, acts, planes, volp, m_two, m_one, share, got1, got2, mid1, mid2,
    load_sem, own_sem, send_sem, recv_sem, red_send, red_recv,
):
    n_gx, n_gy, n_gz = sizes
    n_y = 4
    n_hi = n_gz // n_y
    n_group = n_gx * n_y
    n_line = n_gy * n_hi
    gx, gy, gz = lax.axis_index("gx"), lax.axis_index("gy"), lax.axis_index("gz")
    y_pos, hi_pos = lax.rem(gz, n_y), lax.div(gz, n_y)
    group_at = gx * n_y + y_pos
    line_at = hi_pos * n_gy + gy

    def near(dx, dy, dz):
        return (
            lax.rem(gx + (n_gx + dx), n_gx),
            lax.rem(gy + (n_gy + dy), n_gy),
            lax.rem(gz + (n_gz + dz), n_gz),
        )

    def in_group(k):
        t = lax.rem(group_at + k, n_group)
        return t, (lax.div(t, n_y), gy, hi_pos * n_y + lax.rem(t, n_y))

    def in_line(k):
        t = lax.rem(line_at + k, n_line)
        return t, (gx, lax.rem(t, n_gy), lax.div(t, n_gy) * n_y + y_pos)

    barrier = pltpu.get_barrier_semaphore()
    for dz in (-1, 1, 0):
        for dx in (-1, 0, 1):
            for dy in (-1, 0, 1):
                if (dx, dy, dz) != (0, 0, 0):
                    pl.semaphore_signal(barrier, inc=1, device_id=near(dx, dy, dz), device_id_type=MESH)

    def greet_line(k, _):
        pl.semaphore_signal(barrier, inc=1, device_id=in_line(k)[1], device_id_type=MESH)
        return 0

    def greet_group(k, _):
        pl.semaphore_signal(barrier, inc=1, device_id=in_group(k)[1], device_id_type=MESH)
        return 0

    lax.fori_loop(1, n_line, greet_line, 0)
    lax.fori_loop(1, n_group, greet_group, 0)

    loads = [
        pltpu.make_async_copy(src, dst, load_sem.at[i])
        for i, (src, dst) in enumerate(
            ((cot_h, cot_v), (act2_h, act2_v), (narrow_h, narrow_v), (vol_h, vol_v), (act1_h, act1_v), (wide_h, wide_v), (w2_h, w2_v), (w1_h, w1_v))
        )
    ]
    for copy in loads:
        copy.start()

    def const(name):
        at, n = AT[name]
        return narrow_v[at : at + n, :]

    for i in range(4):
        loads[i].wait()
    perm, eye, ends = const("perm"), const("eye"), const("ends")

    def rows_of(ref, x):
        return ref[:, x].astype(F32).reshape(128, 128)

    def edge_rows(inner_at):
        return jnp.concatenate(
            [inner_at(x)[0:16] for x in range(4)] + [inner_at(x)[112:128] for x in range(4)], axis=0
        )

    row8 = lax.broadcasted_iota(jnp.int32, (8, 128), 0)

    def stack8(rows):
        out = jnp.zeros((8, 128), F32)
        for i, row in enumerate(rows):
            out = jnp.where(row8 == i, jnp.broadcast_to(row, (8, 128)), out)
        return out

    deltas = []
    for x in range(4):
        v = rows_of(cot_v, x)
        deltas.append(jnp.where(rows_of(act2_v, x) > 0, v, v * 0.3).astype(BF16))
    turned = nn(perm, jnp.concatenate(deltas, axis=1))
    bias_two = turned[:, 0:128] + turned[:, 128:256] + turned[:, 256:384] + turned[:, 384:512]
    turned = turned.astype(BF16)
    for x in range(4):
        inner[x] = turned[:, x * 128 : (x + 1) * 128]
    volflat = vol_v[...].astype(F32).reshape(128, 128).astype(BF16)
    vol_tiles = nn(const("tiles"), volflat).astype(BF16)

    def vol_rows(x):
        return vol_v[:, x].astype(F32).reshape(32, 128)

    xs[0, 0:128] = inner[0]
    xs[1, 0:128] = inner[3]
    xs[0, 128:160] = vol_rows(0).astype(BF16)
    xs[1, 128:160] = vol_rows(3).astype(BF16)
    for h in range(2):
        for at, x in ((0, 0), (2, 3), (3, 1), (4, 2)):
            ys[h, at * 16 : at * 16 + 16] = inner[x][112 * h : 112 * h + 16]
        ys[h, 16:32] = vol_tiles[16 * h : 16 * h + 16]
    z_face = nt(ends, jnp.concatenate([inner[x] for x in range(4)], axis=0))
    z_edge = nt(ends, edge_rows(lambda x: inner[x]))
    z_vol = nt(ends, volflat)
    for f in range(2):
        face = [z_face[f : f + 1, x * 128 : (x + 1) * 128] for x in range(4)]
        edge, flat = z_edge[f : f + 1], z_vol[f : f + 1]
        zs[f] = stack8([face[1], face[2], face[0], flat, face[3], edge, flat])

    pl.semaphore_wait(barrier, 26 + (n_line - 1) + (n_group - 1))

    def exchange(phase, xs, xr, ys, yr, xyr, zs, zr):
        first = phase == 0
        out = []

        def send(kind, src, dst, where):
            copy = pltpu.make_async_remote_copy(
                src, dst, send_sem.at[phase, kind], recv_sem.at[phase, kind], device_id=where, device_id_type=MESH
            )
            copy.start()
            out.append(copy)

        for dz in (-1, 1):
            f, side = (1 if dz == 1 else 0), (0 if dz == 1 else 1)
            for dx in (-1, 0, 1):
                for dy in (-1, 0, 1):
                    if first:
                        at, n = {-1: (2, 2), 1: (3, 2), 0: (0, 5) if dy == 0 else (5, 2)}[dx]
                    else:
                        at, n = {-1: (2, 1), 1: (3, 1), 0: (0, 4) if dy == 0 else (4, 1)}[dx]
                    send(0, zs.at[f, pl.ds(at, n)], zr.at[side, pl.ds(8 * way(-dx, -dy), n)], near(dx, dy, dz))
        for dx in (-1, 1):
            send(1, xs.at[(dx + 1) // 2], xr.at[(1 - dx) // 2], near(dx, 0, 0))
        for dy in (-1, 1):
            send(2, ys.at[(dy + 1) // 2], yr.at[(1 - dy) // 2], near(0, dy, 0))
        for dx in (-1, 1):
            for dy in (-1, 1):
                if first:
                    at, n = (0 if dx == -1 else 16), 32
                else:
                    at, n = (0 if dx == -1 else 16), 16
                send(3, ys.at[(dy + 1) // 2, pl.ds(at, n)], xyr.at[corner(-dx, -dy)], near(dx, dy, 0))

    def settle(sems, phase, xr, yr, xyr, zr):
        n = 42 if phase == 0 else 24
        for kind, ref in ((0, zr.at[0, pl.ds(0, n)]), (1, xr), (2, yr), (3, xyr)):
            pltpu.make_async_copy(ref, ref, sems.at[phase, kind]).wait()

    lane_of = lax.broadcasted_iota(jnp.int32, (160, 128), 1)

    def build_planes(phase, inner_at, xr, yr, xyr, zr):
        first = phase == 0
        cols = nt(eye, zr[...].reshape(144, 128).astype(BF16))
        tile_at = {0: 0, 3: 2, 1: 3, 2: 4} if first else {0: 0, 3: 1, 1: 2, 2: 3}
        face_at = {0: 2, 3: 4, 1: 0, 2: 1} if first else {0: 2, 3: 3, 1: 0, 2: 1}
        for p in range(6):
            if 1 <= p <= 4:
                x = p - 1
                low = yr[0, tile_at[x] * 16 : tile_at[x] * 16 + 16]
                mid = inner_at(x)
                high = yr[1, tile_at[x] * 16 : tile_at[x] * 16 + 16]
                pick = (
                    (64 + 16 * x, 80 + 16 * x, 8 * way(0, -1)),
                    (0, 128, 8 * way(0, 0) + face_at[x]),
                    (16 * x, 16 * x + 16, 8 * way(0, 1)),
                )
            else:
                dx = -1 if p == 0 else 1
                at = (16 if dx == -1 else 0) if first else 0
                low = xyr[corner(dx, -1), at : at + 16]
                mid = xr[(dx + 1) // 2, 0:128]
                high = xyr[corner(dx, 1), at : at + 16]
                r = (1 if dx == -1 else 0) if first else 0
                pick = (
                    (112, 128, 8 * way(dx, -1) + r),
                    (0, 128, 8 * way(dx, 0) + r),
                    (0, 16, 8 * way(dx, 1) + r),
                )
            plane = jnp.concatenate([low, mid, high], axis=0)
            lanes = slice(p * 128, (p + 1) * 128)
            planes[160:320, lanes] = plane
            plane = plane.astype(F32)
            for tap, side, turn, lane in ((0, 1, 127, 127), (2, 0, 1, 0)):
                col = jnp.concatenate(
                    [cols[a:b, 72 * side + k : 72 * side + k + 1] for a, b, k in pick], axis=0
                )
                shifted = jnp.where(lane_of == lane, jnp.broadcast_to(col, (160, 128)), pltpu.roll(plane, turn, 1))
                planes[tap * 160 : tap * 160 + 160, lanes] = shifted.astype(BF16)
        return cols

    exchange(0, xs, xr, ys, yr, xyr, zs, zr)

    for i in range(4, 8):
        loads[i].wait()
    turned = nn(perm, jnp.concatenate([rows_of(act1_v, x).astype(BF16) for x in range(4)], axis=1))
    acts[...] = turned.astype(BF16)
    planes[480:512, :] = jnp.zeros((32, 768), BF16)
    place = wide_v[0:48, :]
    band_two = wide_v[48:176, :].astype(F32)
    band_one = wide_v[176:208, :].astype(F32)
    spread = const("spread")[:, 0:16]
    for a in range(3):
        total_two = jnp.zeros((128, 512), F32)
        total_one = jnp.zeros((32, 512), F32)
        for b in range(3):
            t = (a * 3 + b) * 3
            group = w2_v[t : t + 3].reshape(48, 16)
            wide = nn(nt(spread, group).astype(BF16), place)
            total_two = jnp.where(band_two == b, wide, total_two)
            four = jnp.zeros((4, 512), F32)
            for c in range(3):
                four = four + nn(w1_v[t + c], place[c * 16 : c * 16 + 16])
            wide = jnp.concatenate([jnp.broadcast_to(four[j : j + 1], (8, 512)) for j in range(4)], axis=0)
            total_one = jnp.where(band_one == b, wide, total_one)
        m_two[a] = total_two.astype(BF16)
        m_one[a] = total_one.astype(BF16)

    settle(recv_sem, 0, xr, yr, xyr, zr)
    cols = build_planes(0, lambda x: inner[x], xr, yr, xyr, zr)

    back = nn(m_two[0], planes[:, 256:768]) + nn(m_two[1], planes[:, 128:640]) + nn(m_two[2], planes[:, 0:512])
    delta = jnp.where(acts[...].astype(F32) > 0, back, back * 0.3).astype(BF16)
    wide_delta = delta.astype(F32)
    bias_one = wide_delta[:, 0:128] + wide_delta[:, 128:256] + wide_delta[:, 256:384] + wide_delta[:, 384:512]

    def delta_at(x):
        return delta[:, x * 128 : (x + 1) * 128]

    xs2[0] = delta_at(0)
    xs2[1] = delta_at(3)
    for h in range(2):
        for at, x in ((0, 0), (1, 3), (2, 1), (3, 2)):
            ys2[h, at * 16 : at * 16 + 16] = delta_at(x)[112 * h : 112 * h + 16]
    z_face = nt(ends, jnp.concatenate([delta_at(x) for x in range(4)], axis=0))
    z_edge = nt(ends, edge_rows(delta_at))
    for f in range(2):
        face = [z_face[f : f + 1, x * 128 : (x + 1) * 128] for x in range(4)]
        zs2[f] = stack8([face[1], face[2], face[0], face[3], z_edge[f : f + 1]])
    exchange(1, xs2, xr2, ys2, yr2, xyr2, zs2, zr2)
    for x in range(4):
        inner[x] = delta_at(x)

    v_tiles = jnp.concatenate(
        [yr[0, 16:32], yr[1, 16:32]]
        + [xyr[corner(dx, dy), at : at + 16] for dx, at in ((-1, 0), (1, 16)) for dy in (-1, 1)],
        axis=0,
    )
    rims = nn(const("rim_rows")[:, 0:96], v_tiles)
    rim_cols = nn(const("rim_cols"), cols.astype(BF16))
    lane40 = lax.broadcasted_iota(jnp.int32, (40, 128), 1)
    half8 = lax.broadcasted_iota(jnp.int32, (8, 1), 0) < 4
    volp[120:128, :] = jnp.zeros((8, 768), F32)
    for p in range(6):
        x = (p - 1) % 4
        dx = -1 if p == 0 else (1 if p == 5 else 0)
        mid = vol_rows(x) if dx == 0 else xr[(dx + 1) // 2, 128:160].astype(F32)
        plane = jnp.concatenate([mid, rims[p * 8 : p * 8 + 8]], axis=0)
        lanes = slice(p * 128, (p + 1) * 128)
        volp[40:80, lanes] = plane
        r = {-1: 0, 1: 1, 0: 1}[dx]
        for tap, side, turn, lane in ((0, 0, 1, 0), (2, 1, 127, 127)):
            k = 72 * side + 8 * way(dx, 0) + (3 if dx == 0 else r)
            col = jnp.concatenate(
                [cols[j * 32 + x * 8 : j * 32 + x * 8 + 8, k : k + 1] for j in range(4)]
                + [
                    jnp.where(
                        half8,
                        rim_cols[p * 8 : p * 8 + 8, 72 * side + 8 * way(dx, -1) + r : 72 * side + 8 * way(dx, -1) + r + 1],
                        rim_cols[p * 8 : p * 8 + 8, 72 * side + 8 * way(dx, 1) + r : 72 * side + 8 * way(dx, 1) + r + 1],
                    )
                ],
                axis=0,
            )
            volp[tap * 40 : tap * 40 + 40, lanes] = jnp.where(
                lane40 == lane, jnp.broadcast_to(col, (40, 128)), pltpu.roll(plane, turn, 1)
            )

    y_of = const("y_of").astype(F32)
    sums = []
    for a in range(3):
        g = nt(delta, volp[:, a * 128 : (a + 4) * 128].astype(BF16))
        for b in range(3):
            total = jnp.zeros((16, 128), F32)
            for y in range(8):
                total = total + jnp.where(y_of == y + b, g[y * 16 : y * 16 + 16], 0.0)
            sums.append(total)
    sums = jnp.concatenate(sums, axis=1)
    top = sums.astype(BF16)
    rest = (sums - top.astype(F32)).astype(BF16)
    fold = const("fold")
    packed = nn(top, fold) + nn(rest, fold)

    def fold_y(v):
        out = v[0:16]
        for y in range(1, 8):
            out = out + v[y * 16 : y * 16 + 16]
        return jnp.broadcast_to(jnp.sum(out, axis=1, keepdims=True), (16, 128))

    lane16 = lax.broadcasted_iota(jnp.int32, (16, 128), 1)
    share[64:80] = jnp.where(lane16 >= 108, fold_y(bias_one), packed)
    share[80:96] = jnp.zeros((16, 128), F32)

    slot = lax.shift_right_logical(lane16, 4)
    blocks = [jnp.zeros((16, 128), F32) for _ in range(4)]
    for a in range(3):
        g = nt(planes[0:480, (2 - a) * 128 : (6 - a) * 128], acts[...])
        for b in range(3):
            for c in range(3):
                t = (a * 3 + b) * 3 + c
                total = jnp.zeros((16, 128), F32)
                for y in range(8):
                    at = c * 160 + (y + 2 - b) * 16
                    total = jnp.where(slot == y, g[at : at + 16], total)
                for turn in (64, 32, 16):
                    total = total + pltpu.roll(total, turn, 1)
                blocks[t // 8] = jnp.where(slot == t % 8, total, blocks[t // 8])
    blocks[3] = jnp.where(slot == 3, fold_y(bias_two), blocks[3])
    for k in range(4):
        share[k * 16 : k * 16 + 16] = blocks[k]

    def scatter(k, _):
        t, where = in_group(k)
        pltpu.make_async_remote_copy(
            share.at[pl.ds(ROWS * t, ROWS)], got1.at[pl.ds(4 * group_at, ROWS)],
            red_send.at[0], red_recv.at[0], device_id=where, device_id_type=MESH,
        ).start()
        return 0

    lax.fori_loop(1, n_group, scatter, 0)
    own = pltpu.make_async_copy(share.at[pl.ds(ROWS * group_at, ROWS)], got1.at[pl.ds(4 * group_at, ROWS)], own_sem.at[0])
    own.start()
    own.wait()

    def await_rows(sem, ref, n):
        ref = ref.at[pl.ds(0, n * ROWS)]
        pltpu.make_async_copy(ref, ref, sem).wait()

    def total8(ref, n):
        out = ref[0:8]
        for i in range(1, n // 2):
            out = out + ref[i * 8 : i * 8 + 8]
        return out + pltpu.roll(out, 4, 0)

    await_rows(red_recv.at[0], got1, n_group - 1)
    mid1[...] = total8(got1, n_group)

    def along(k, _):
        _, where = in_line(k)
        pltpu.make_async_remote_copy(
            mid1.at[pl.ds(0, ROWS)], got2.at[pl.ds(4 * line_at, ROWS)],
            red_send.at[1], red_recv.at[1], device_id=where, device_id_type=MESH,
        ).start()
        return 0

    lax.fori_loop(1, n_line, along, 0)
    own = pltpu.make_async_copy(mid1.at[pl.ds(0, ROWS)], got2.at[pl.ds(4 * line_at, ROWS)], own_sem.at[1])
    own.start()
    own.wait()

    settle(recv_sem, 1, xr2, yr2, xyr2, zr2)
    build_planes(1, lambda x: inner[x], xr2, yr2, xyr2, zr2)
    grad = nn(m_one[0], planes[:, 256:768]) + nn(m_one[1], planes[:, 128:640]) + nn(m_one[2], planes[:, 0:512])
    for j in range(4):
        for x in range(4):
            gvol[j, x] = grad[j * 8 : j * 8 + 8, x * 128 : (x + 1) * 128]

    await_rows(red_recv.at[1], got2, n_line - 1)
    mid2[...] = total8(got2, n_line) * norm

    def gather(k, _):
        _, where = in_group(k)
        pltpu.make_async_remote_copy(
            mid2.at[pl.ds(0, ROWS)], summed.at[pl.ds(ROWS * group_at, ROWS)],
            red_send.at[2], red_recv.at[2], device_id=where, device_id_type=MESH,
        ).start()
        return 0

    lax.fori_loop(1, n_group, gather, 0)
    own = pltpu.make_async_copy(mid2.at[pl.ds(0, ROWS)], summed.at[pl.ds(ROWS * group_at, ROWS)], own_sem.at[2])
    own.start()
    own.wait()
    settle(send_sem, 0, xr, yr, xyr, zr)
    settle(send_sem, 1, xr2, yr2, xyr2, zr2)
    await_rows(red_send.at[0], got1, n_group - 1)
    await_rows(red_send.at[1], got2, n_line - 1)
    await_rows(red_recv.at[2], summed, n_group - 1)

    await_rows(red_send.at[2], summed, n_group - 1)


def finish(
    summed, gvol_v, gw1, gb1, gw2, gb2, gvol,
    gw1_v, gb1_v, gw2_v, gb2_v, sems,
):
    copies = [
        pltpu.make_async_copy(src, dst, sems.at[i])
        for i, (src, dst) in enumerate(((gvol_v, gvol), (gw2_v, gw2), (gw1_v, gw1), (gb1_v, gb1), (gb2_v, gb2)))
    ]
    copies[0].start()
    for k in range(4):
        block = summed[k * 16 : k * 16 + 16]
        for s in range(8):
            if k * 8 + s < 27:
                turned = pltpu.roll(block, (128 - 16 * s) % 128, 1) if s else block
                gw2_v[k * 8 + s] = turned[:, 0:16]
    copies[1].start()
    packed = summed[64:80].T
    for t in range(27):
        gw1_v[t] = packed[4 * t : 4 * t + 4, :]
    copies[2].start()
    gb1_v[...] = packed[108, :]
    gb2_v[...] = summed[48:64].T[48, :]
    copies[3].start()
    copies[4].start()
    for copy in copies:
        copy.wait()


def local(sizes, norm, volume, act_one, act_two, weight_one, weight_two, cotangent):
    narrow, wide = constants()
    w1 = jnp.transpose(weight_one, (2, 3, 4, 1, 0)).reshape(27, CHAN_IN, CHAN)
    w2 = jnp.transpose(weight_two, (2, 3, 4, 0, 1)).reshape(27, CHAN, CHAN)
    n_group = sizes[0] * 4
    n_line = sizes[1] * (sizes[2] // 4)
    buf = lambda *shape: pltpu.VMEM(shape, BF16)
    buf32 = lambda *shape: pltpu.VMEM(shape, F32)
    block = (CHAN, NX, NY, NZ)
    summed, gvol = pl.pallas_call(
        functools.partial(kernel, sizes, norm),
        out_shape=(
            pltpu.VMEM((96, 128), F32),
            pltpu.VMEM((CHAN_IN, NX, NY, NZ), F32),
        ),
        in_specs=[pl.BlockSpec(memory_space=pl.ANY)] * 8,
        out_specs=tuple([pl.BlockSpec(memory_space=pltpu.VMEM)] * 2),
        scratch_shapes=[
            buf(CHAN_IN, NX, NY, NZ), buf(*block), buf(*block), buf(27, CHAN_IN, CHAN), buf(27, CHAN, CHAN), buf(*block),
            buf(NARROW, 128), buf(208, 512),
            buf(2, 160, 128), buf(2, 160, 128), buf(2, 80, 128), buf(2, 80, 128), buf(4, 32, 128), buf32(2, 8, 128), buf32(2, 72, 128),
            buf(2, 128, 128), buf(2, 128, 128), buf(2, 64, 128), buf(2, 64, 128), buf(4, 16, 128), buf32(2, 8, 128), buf32(2, 72, 128),
            buf(4, 128, 128), buf(128, 512), buf(512, 768), buf32(128, 768), buf(3, 128, 512), buf(3, 32, 512),
            buf32(96, 128), buf32(4 * n_group, 128), buf32(4 * n_line, 128), buf32(8, 128), buf32(8, 128),
            pltpu.SemaphoreType.DMA((8,)), pltpu.SemaphoreType.DMA((3,)),
            pltpu.SemaphoreType.DMA((2, 4)), pltpu.SemaphoreType.DMA((2, 4)),
            pltpu.SemaphoreType.DMA((3,)), pltpu.SemaphoreType.DMA((3,)),
        ],
        compiler_params=pltpu.CompilerParams(collective_id=0, has_side_effects=True, vmem_limit_bytes=60 * 2**20),
        name="both_layers",
    )(volume, act_one, act_two, w1, w2, cotangent, narrow, wide)
    shapes = ((27, CHAN_IN, CHAN), (CHAN,), (27, CHAN, CHAN), (CHAN,))
    gw1, gb1, gw2, gb2, gvol = pl.pallas_call(
        finish,
        out_shape=tuple(jax.ShapeDtypeStruct(shape, F32) for shape in shapes + ((CHAN_IN, NX, NY, NZ),)),
        in_specs=[pl.BlockSpec(memory_space=pltpu.VMEM)] * 2,
        out_specs=tuple([pl.BlockSpec(memory_space=pl.ANY)] * 5),
        scratch_shapes=[buf32(*shape) for shape in shapes] + [pltpu.SemaphoreType.DMA((5,))],
        compiler_params=pltpu.CompilerParams(vmem_limit_bytes=8 * 2**20),
        name="finish",
    )(summed, gvol)
    gw1 = jnp.transpose(gw1.reshape(3, 3, 3, CHAN_IN, CHAN), (4, 3, 0, 1, 2))
    gw2 = jnp.transpose(gw2.reshape(3, 3, 3, CHAN, CHAN), (3, 4, 0, 1, 2))
    return gw1, gb1, gw2, gb2, gvol


def solution(mesh):
    sizes = tuple(mesh.shape[name] for name in ("gx", "gy", "gz"))
    norm = 1.0 / math.sqrt(NX * NY * NZ * sizes[0] * sizes[1] * sizes[2])
    block = P(None, "gx", "gy", "gz")
    return jax.shard_map(
        functools.partial(local, sizes, norm),
        mesh=mesh,
        in_specs=(block, block, block, P(), P(), block),
        out_specs=(P(), P(), P(), P(), block),
        check_vma=False,
    )
```

```python
import functools
import math

import jax
import jax.numpy as jnp
import numpy as np
from jax import lax
from jax.experimental import pallas as pl
from jax.experimental.pallas import tpu as pltpu
from jax.sharding import PartitionSpec as P

CHAN_IN = 4
CHAN = 16
NX, NY, NZ = 4, 8, 128
F32, BF16 = jnp.float32, jnp.bfloat16
MESH = pl.DeviceIdType.MESH
ROWS = 3
SIDES = ((-1, 0), (1, 0), (0, -1), (0, 1), (-1, -1), (-1, 1), (1, -1), (1, 1))


def constants():
    r = np.arange(128)
    perm = np.zeros((128, 128), np.float32)
    perm[r, (r % 16) * 8 + r // 16] = 1
    eye = np.eye(128, dtype=np.float32)
    ends = np.zeros((16, 128), np.float32)
    ends[0, 0] = ends[1, 127] = 1
    tiles = np.zeros((32, 128), np.float32)
    for h in range(2):
        for x in range(4):
            for j in range(4):
                tiles[h * 16 + x * 4 + j, j * 32 + x * 8 + 7 * h] = 1
    rim_cols = np.zeros((48, 128), np.float32)
    rim_rows = np.zeros((48, 128), np.float32)
    for p in range(6):
        x = (p - 1) % 4
        for h in range(2):
            for j in range(4):
                rim_cols[p * 8 + h * 4 + j, j * 32 + x * 8 + 7 * (1 - h)] = 1
                tile = h if 1 <= p <= 4 else 2 + (0 if p == 0 else 2) + h
                rim_rows[p * 8 + h * 4 + j, tile * 16 + x * 4 + j] = 1
    spread = np.zeros((128, 128), np.float32)
    spread[r, r % 16] = 1
    narrow = np.concatenate([perm, eye, ends, tiles, rim_cols, rim_rows, spread])
    lane = np.arange(512)
    inside = lane < 480
    tap, end, chan = lane // 160, (lane % 160) // 16, lane % 16
    place = np.zeros((48, 512), np.float32)
    for c in range(3):
        for o in range(16):
            place[c * 16 + o] = inside & (tap == c) & (chan == o)
    y_two = (np.arange(128) // 16)[:, None]
    y_one = (np.arange(32) % 8)[:, None]
    band_two = np.where(inside[None], y_two + 2 - end[None], -9)
    band_one = np.where(inside[None], y_one + 2 - end[None], -9)
    wide = np.concatenate([place, band_two, band_one])
    rr = np.arange(128) % 40
    ok = np.arange(128) < 120
    row_y = np.where(rr < 32, 1 + rr % 8, np.where(rr < 36, 0, 9))
    row_j = np.where(rr < 32, rr // 8, rr % 4)
    row_c = np.arange(128) // 40
    y_of = np.broadcast_to(np.where(ok, row_y, -9)[None], (16, 128))
    fold = np.zeros((9, 128, 128), np.float32)
    for ab in range(9):
        for q in range(120):
            fold[ab, q, (ab * 3 + row_c[q]) * 4 + row_j[q]] = 1
    narrow = np.concatenate([narrow, y_of])
    return jnp.asarray(narrow, BF16), jnp.asarray(wide, BF16), jnp.asarray(fold.reshape(-1, 128), BF16)


AT = {}
_at = 0
for _name, _n in (("perm", 128), ("eye", 128), ("ends", 16), ("tiles", 32), ("rim_cols", 48), ("rim_rows", 48), ("spread", 128), ("y_of", 16)):
    AT[_name] = (_at, _n)
    _at += _n
NARROW = _at


def nt(a, b):
    return lax.dot_general(a, b, (((1,), (1,)), ((), ())), preferred_element_type=F32)


def nn(a, b):
    return jnp.dot(a, b, preferred_element_type=F32)


def way(dx, dy):
    return (dx + 1) * 3 + dy + 1


def corner(dx, dy):
    return (dx + 1) + (dy + 1) // 2


def kernel(
    sizes, norm,
    vol_h, act1_h, act2_h, w1_h, w2_h, cot_h, narrow_h, wide_h, fold_h,
    summed, gvol,
    vol_v, act1_v, act2_v, w1_v, w2_v, cot_v, narrow_v, wide_v, fold_v,
    xs, xr, ys, yr, xyr, zs, zr,
    xs2, xr2, ys2, yr2, xyr2, zs2, zr2,
    inner, acts, planes, volp, m_two, m_one, share, got1, got2, mid1, mid2,
    load_sem, own_sem, send_sem, recv_sem, red_send, red_recv,
):
    n_gx, n_gy, n_gz = sizes
    n_y = 4
    n_hi = n_gz // n_y
    n_group = n_gx * n_y
    n_line = n_gy * n_hi
    gx, gy, gz = lax.axis_index("gx"), lax.axis_index("gy"), lax.axis_index("gz")
    y_pos, hi_pos = lax.rem(gz, n_y), lax.div(gz, n_y)
    group_at = gx * n_y + y_pos
    line_at = hi_pos * n_gy + gy

    loads = [
        pltpu.make_async_copy(src, dst, load_sem.at[i])
        for i, (src, dst) in enumerate(
            ((cot_h, cot_v), (act2_h, act2_v), (narrow_h, narrow_v), (vol_h, vol_v), (act1_h, act1_v), (wide_h, wide_v), (w2_h, w2_v), (w1_h, w1_v), (fold_h, fold_v))
        )
    ]
    for copy in loads[:4]:
        copy.start()

    gx_at = [lax.rem(gx + d, n_gx) for d in range(n_gx)]
    gy_at = [lax.rem(gy + d, n_gy) for d in range(n_gy)]
    gz_at = [lax.rem(gz + d, n_gz) for d in range(n_gz)]
    y_at = [lax.rem(y_pos + d, n_y) for d in range(n_y)]
    line_to = [lax.rem(line_at + d, n_line) for d in range(n_line)]
    run_base = hi_pos * n_y

    def near(dx, dy, dz):
        return gx_at[dx], gy_at[dy], gz_at[dz]

    def ring(d, n):
        return min(d, n - d)

    group_steps = sorted(
        ((d, e) for d in range(n_gx) for e in range(n_y) if (d, e) != (0, 0)),
        key=lambda p: -(ring(p[0], n_gx) / 2 + ring(p[1], n_y)),
    )
    line_steps = sorted(range(1, n_line), key=lambda d: -ring(d, n_line))

    def in_group(step):
        d, e = step
        return gx_at[d] * n_y + y_at[e], (gx_at[d], gy, run_base + y_at[e])

    def in_line(d):
        return gx, lax.rem(line_to[d], n_gy), lax.div(line_to[d], n_gy) * n_y + y_pos

    barrier = pltpu.get_barrier_semaphore()
    for dz in (-1, 1, 0):
        for dx in (-1, 0, 1):
            for dy in (-1, 0, 1):
                if (dx, dy, dz) != (0, 0, 0):
                    pl.semaphore_signal(barrier, inc=1, device_id=near(dx, dy, dz), device_id_type=MESH)

    for d in line_steps:
        pl.semaphore_signal(barrier, inc=1, device_id=in_line(d), device_id_type=MESH)
    for step in group_steps:
        pl.semaphore_signal(barrier, inc=1, device_id=in_group(step)[1], device_id_type=MESH)
    for copy in loads[4:]:
        copy.start()

    def const(name):
        at, n = AT[name]
        return narrow_v[at : at + n, :]

    for i in range(4):
        loads[i].wait()
    perm, eye, ends = const("perm"), const("eye"), const("ends")

    def rows_of(ref, x):
        return ref[:, x].astype(F32).reshape(128, 128)

    def edge_rows(inner_at):
        return jnp.concatenate(
            [inner_at(x)[0:16] for x in range(4)] + [inner_at(x)[112:128] for x in range(4)], axis=0
        )

    row8 = lax.broadcasted_iota(jnp.int32, (8, 128), 0)

    def stack8(rows):
        out = jnp.zeros((8, 128), F32)
        for i, row in enumerate(rows):
            out = jnp.where(row8 == i, jnp.broadcast_to(row, (8, 128)), out)
        return out

    deltas = []
    for x in range(4):
        v = rows_of(cot_v, x)
        deltas.append(jnp.where(rows_of(act2_v, x) > 0, v, v * 0.3).astype(BF16))
    turned = nn(perm, jnp.concatenate(deltas, axis=1))
    bias_two = turned[:, 0:128] + turned[:, 128:256] + turned[:, 256:384] + turned[:, 384:512]
    turned = turned.astype(BF16)
    for x in range(4):
        inner[x] = turned[:, x * 128 : (x + 1) * 128]
    volflat = vol_v[...].astype(F32).reshape(128, 128).astype(BF16)
    vol_tiles = nn(const("tiles"), volflat).astype(BF16)

    def vol_rows(x):
        return vol_v[:, x].astype(F32).reshape(32, 128)

    xs[0, 0:128] = inner[0]
    xs[1, 0:128] = inner[3]
    xs[0, 128:160] = vol_rows(0).astype(BF16)
    xs[1, 128:160] = vol_rows(3).astype(BF16)
    for h in range(2):
        for at, x in ((0, 0), (2, 3), (3, 1), (4, 2)):
            ys[h, at * 16 : at * 16 + 16] = inner[x][112 * h : 112 * h + 16]
        ys[h, 16:32] = vol_tiles[16 * h : 16 * h + 16]
    z_face = nt(ends, jnp.concatenate([inner[x] for x in range(4)], axis=0))
    z_edge = nt(ends, edge_rows(lambda x: inner[x]))
    z_vol = nt(ends, volflat)
    for f in range(2):
        face = [z_face[f : f + 1, x * 128 : (x + 1) * 128] for x in range(4)]
        edge, flat = z_edge[f : f + 1], z_vol[f : f + 1]
        zs[f] = stack8([face[1], face[2], face[0], flat, face[3], edge, flat])

    pl.semaphore_wait(barrier, 26 + (n_line - 1) + (n_group - 1))

    def exchange(phase, xs, xr, ys, yr, xyr, zs, zr):
        first = phase == 0
        out = []

        def send(kind, src, dst, where):
            copy = pltpu.make_async_remote_copy(
                src, dst, send_sem.at[phase, kind], recv_sem.at[phase, kind], device_id=where, device_id_type=MESH
            )
            copy.start()
            out.append(copy)

        for dz in (-1, 1):
            f, side = (1 if dz == 1 else 0), (0 if dz == 1 else 1)
            for dx in (-1, 0, 1):
                for dy in (-1, 0, 1):
                    if first:
                        at, n = {-1: (2, 2), 1: (3, 2), 0: (0, 5) if dy == 0 else (5, 2)}[dx]
                    else:
                        at, n = {-1: (2, 1), 1: (3, 1), 0: (0, 4) if dy == 0 else (4, 1)}[dx]
                    send(0, zs.at[f, pl.ds(at, n)], zr.at[side, pl.ds(8 * way(-dx, -dy), n)], near(dx, dy, dz))
        for dx in (-1, 1):
            send(1, xs.at[(dx + 1) // 2], xr.at[(1 - dx) // 2], near(dx, 0, 0))
        for dy in (-1, 1):
            send(2, ys.at[(dy + 1) // 2], yr.at[(1 - dy) // 2], near(0, dy, 0))
        for dx in (-1, 1):
            for dy in (-1, 1):
                if first:
                    at, n = (0 if dx == -1 else 16), 32
                else:
                    at, n = (0 if dx == -1 else 16), 16
                send(3, ys.at[(dy + 1) // 2, pl.ds(at, n)], xyr.at[corner(-dx, -dy)], near(dx, dy, 0))

    def settle(sems, phase, xr, yr, xyr, zr):
        n = 42 if phase == 0 else 24
        for kind, ref in ((0, zr.at[0, pl.ds(0, n)]), (1, xr), (2, yr), (3, xyr)):
            pltpu.make_async_copy(ref, ref, sems.at[phase, kind]).wait()

    lane_of = lax.broadcasted_iota(jnp.int32, (160, 128), 1)

    def build_planes(phase, inner_at, xr, yr, xyr, zr):
        first = phase == 0
        cols = nt(eye, zr[...].reshape(144, 128).astype(BF16))
        tile_at = {0: 0, 3: 2, 1: 3, 2: 4} if first else {0: 0, 3: 1, 1: 2, 2: 3}
        face_at = {0: 2, 3: 4, 1: 0, 2: 1} if first else {0: 2, 3: 3, 1: 0, 2: 1}
        for p in range(6):
            if 1 <= p <= 4:
                x = p - 1
                low = yr[0, tile_at[x] * 16 : tile_at[x] * 16 + 16]
                mid = inner_at(x)
                high = yr[1, tile_at[x] * 16 : tile_at[x] * 16 + 16]
                pick = (
                    (64 + 16 * x, 80 + 16 * x, 8 * way(0, -1)),
                    (0, 128, 8 * way(0, 0) + face_at[x]),
                    (16 * x, 16 * x + 16, 8 * way(0, 1)),
                )
            else:
                dx = -1 if p == 0 else 1
                at = (16 if dx == -1 else 0) if first else 0
                low = xyr[corner(dx, -1), at : at + 16]
                mid = xr[(dx + 1) // 2, 0:128]
                high = xyr[corner(dx, 1), at : at + 16]
                r = (1 if dx == -1 else 0) if first else 0
                pick = (
                    (112, 128, 8 * way(dx, -1) + r),
                    (0, 128, 8 * way(dx, 0) + r),
                    (0, 16, 8 * way(dx, 1) + r),
                )
            plane = jnp.concatenate([low, mid, high], axis=0)
            lanes = slice(p * 128, (p + 1) * 128)
            planes[160:320, lanes] = plane
            plane = plane.astype(F32)
            for tap, side, turn, lane in ((0, 1, 127, 127), (2, 0, 1, 0)):
                col = jnp.concatenate(
                    [cols[a:b, 72 * side + k : 72 * side + k + 1] for a, b, k in pick], axis=0
                )
                shifted = jnp.where(lane_of == lane, jnp.broadcast_to(col, (160, 128)), pltpu.roll(plane, turn, 1))
                planes[tap * 160 : tap * 160 + 160, lanes] = shifted.astype(BF16)
        return cols

    exchange(0, xs, xr, ys, yr, xyr, zs, zr)

    for i in range(4, 9):
        loads[i].wait()
    turned = nn(perm, jnp.concatenate([rows_of(act1_v, x).astype(BF16) for x in range(4)], axis=1))
    acts[...] = turned.astype(BF16)
    planes[480:512, :] = jnp.zeros((32, 768), BF16)
    place = wide_v[0:48, :]
    band_two = wide_v[48:176, :].astype(F32)
    band_one = wide_v[176:208, :].astype(F32)
    spread = const("spread")[:, 0:16]
    for a in range(3):
        total_two = jnp.zeros((128, 512), F32)
        total_one = jnp.zeros((32, 512), F32)
        for b in range(3):
            t = (a * 3 + b) * 3
            group = w2_v[t : t + 3].reshape(48, 16)
            wide = nn(nt(spread, group).astype(BF16), place)
            total_two = jnp.where(band_two == b, wide, total_two)
            four = jnp.zeros((4, 512), F32)
            for c in range(3):
                four = four + nn(w1_v[t + c], place[c * 16 : c * 16 + 16])
            wide = jnp.concatenate([jnp.broadcast_to(four[j : j + 1], (8, 512)) for j in range(4)], axis=0)
            total_one = jnp.where(band_one == b, wide, total_one)
        m_two[a] = total_two.astype(BF16)
        m_one[a] = total_one.astype(BF16)

    settle(recv_sem, 0, xr, yr, xyr, zr)
    cols = build_planes(0, lambda x: inner[x], xr, yr, xyr, zr)

    back = nn(m_two[0], planes[:, 256:768]) + nn(m_two[1], planes[:, 128:640]) + nn(m_two[2], planes[:, 0:512])
    delta = jnp.where(acts[...].astype(F32) > 0, back, back * 0.3).astype(BF16)
    wide_delta = delta.astype(F32)
    bias_one = wide_delta[:, 0:128] + wide_delta[:, 128:256] + wide_delta[:, 256:384] + wide_delta[:, 384:512]

    def delta_at(x):
        return delta[:, x * 128 : (x + 1) * 128]

    xs2[0] = delta_at(0)
    xs2[1] = delta_at(3)
    for h in range(2):
        for at, x in ((0, 0), (1, 3), (2, 1), (3, 2)):
            ys2[h, at * 16 : at * 16 + 16] = delta_at(x)[112 * h : 112 * h + 16]
    z_face = nt(ends, jnp.concatenate([delta_at(x) for x in range(4)], axis=0))
    z_edge = nt(ends, edge_rows(delta_at))
    for f in range(2):
        face = [z_face[f : f + 1, x * 128 : (x + 1) * 128] for x in range(4)]
        zs2[f] = stack8([face[1], face[2], face[0], face[3], z_edge[f : f + 1]])
    exchange(1, xs2, xr2, ys2, yr2, xyr2, zs2, zr2)
    for x in range(4):
        inner[x] = delta_at(x)

    v_tiles = jnp.concatenate(
        [yr[0, 16:32], yr[1, 16:32]]
        + [xyr[corner(dx, dy), at : at + 16] for dx, at in ((-1, 0), (1, 16)) for dy in (-1, 1)],
        axis=0,
    )
    rims = nn(const("rim_rows")[:, 0:96], v_tiles)
    rim_cols = nn(const("rim_cols"), cols.astype(BF16))
    lane40 = lax.broadcasted_iota(jnp.int32, (40, 128), 1)
    half8 = lax.broadcasted_iota(jnp.int32, (8, 1), 0) < 4
    volp[120:128, :] = jnp.zeros((8, 768), F32)
    for p in range(6):
        x = (p - 1) % 4
        dx = -1 if p == 0 else (1 if p == 5 else 0)
        mid = vol_rows(x) if dx == 0 else xr[(dx + 1) // 2, 128:160].astype(F32)
        plane = jnp.concatenate([mid, rims[p * 8 : p * 8 + 8]], axis=0)
        lanes = slice(p * 128, (p + 1) * 128)
        volp[40:80, lanes] = plane
        r = {-1: 0, 1: 1, 0: 1}[dx]
        for tap, side, turn, lane in ((0, 0, 1, 0), (2, 1, 127, 127)):
            k = 72 * side + 8 * way(dx, 0) + (3 if dx == 0 else r)
            col = jnp.concatenate(
                [cols[j * 32 + x * 8 : j * 32 + x * 8 + 8, k : k + 1] for j in range(4)]
                + [
                    jnp.where(
                        half8,
                        rim_cols[p * 8 : p * 8 + 8, 72 * side + 8 * way(dx, -1) + r : 72 * side + 8 * way(dx, -1) + r + 1],
                        rim_cols[p * 8 : p * 8 + 8, 72 * side + 8 * way(dx, 1) + r : 72 * side + 8 * way(dx, 1) + r + 1],
                    )
                ],
                axis=0,
            )
            volp[tap * 40 : tap * 40 + 40, lanes] = jnp.where(
                lane40 == lane, jnp.broadcast_to(col, (40, 128)), pltpu.roll(plane, turn, 1)
            )

    y_of = const("y_of").astype(F32)
    sums = []
    for a in range(3):
        g = nt(delta, volp[:, a * 128 : (a + 4) * 128].astype(BF16))
        for b in range(3):
            total = jnp.zeros((16, 128), F32)
            for y in range(8):
                total = total + jnp.where(y_of == y + b, g[y * 16 : y * 16 + 16], 0.0)
            sums.append(total)
    sums = jnp.concatenate(sums, axis=1)
    top = sums.astype(BF16)
    rest = (sums - top.astype(F32)).astype(BF16)
    fold = fold_v[...]
    packed = nn(top, fold) + nn(rest, fold)

    def fold_y(v):
        out = v[0:16]
        for y in range(1, 8):
            out = out + v[y * 16 : y * 16 + 16]
        return jnp.broadcast_to(jnp.sum(out, axis=1, keepdims=True), (16, 128))

    lane16 = lax.broadcasted_iota(jnp.int32, (16, 128), 1)
    share[64:80] = jnp.where(lane16 >= 108, fold_y(bias_one), packed)
    share[80:96] = jnp.zeros((16, 128), F32)

    slot = lax.shift_right_logical(lane16, 4)
    blocks = [jnp.zeros((16, 128), F32) for _ in range(4)]
    for a in range(3):
        g = nt(planes[0:480, (2 - a) * 128 : (6 - a) * 128], acts[...])
        for b in range(3):
            for c in range(3):
                t = (a * 3 + b) * 3 + c
                total = jnp.zeros((16, 128), F32)
                for y in range(8):
                    at = c * 160 + (y + 2 - b) * 16
                    total = jnp.where(slot == y, g[at : at + 16], total)
                for turn in (64, 32, 16):
                    total = total + pltpu.roll(total, turn, 1)
                blocks[t // 8] = jnp.where(slot == t % 8, total, blocks[t // 8])
    blocks[3] = jnp.where(slot == 3, fold_y(bias_two), blocks[3])
    for k in range(4):
        share[k * 16 : k * 16 + 16] = blocks[k]

    for step in group_steps:
        t, where = in_group(step)
        pltpu.make_async_remote_copy(
            share.at[pl.ds(ROWS * t, ROWS)], got1.at[pl.ds(4 * group_at, ROWS)],
            red_send.at[0], red_recv.at[0], device_id=where, device_id_type=MESH,
        ).start()
    own = pltpu.make_async_copy(share.at[pl.ds(ROWS * group_at, ROWS)], got1.at[pl.ds(4 * group_at, ROWS)], own_sem.at[0])
    own.start()
    own.wait()

    def await_rows(sem, ref, n):
        ref = ref.at[pl.ds(0, n * ROWS)]
        pltpu.make_async_copy(ref, ref, sem).wait()

    def total8(ref, n):
        out = ref[0:8]
        for i in range(1, n // 2):
            out = out + ref[i * 8 : i * 8 + 8]
        return out + pltpu.roll(out, 4, 0)

    await_rows(red_recv.at[0], got1, n_group - 1)
    mid1[...] = total8(got1, n_group)

    for d in line_steps:
        pltpu.make_async_remote_copy(
            mid1.at[pl.ds(0, ROWS)], got2.at[pl.ds(4 * line_at, ROWS)],
            red_send.at[1], red_recv.at[1], device_id=in_line(d), device_id_type=MESH,
        ).start()
    own = pltpu.make_async_copy(mid1.at[pl.ds(0, ROWS)], got2.at[pl.ds(4 * line_at, ROWS)], own_sem.at[1])
    own.start()
    own.wait()

    settle(recv_sem, 1, xr2, yr2, xyr2, zr2)
    build_planes(1, lambda x: inner[x], xr2, yr2, xyr2, zr2)
    grad = nn(m_one[0], planes[:, 256:768]) + nn(m_one[1], planes[:, 128:640]) + nn(m_one[2], planes[:, 0:512])
    for j in range(4):
        for x in range(4):
            gvol[j, x] = grad[j * 8 : j * 8 + 8, x * 128 : (x + 1) * 128]

    await_rows(red_recv.at[1], got2, n_line - 1)
    mid2[...] = total8(got2, n_line) * norm

    for step in group_steps:
        pltpu.make_async_remote_copy(
            mid2.at[pl.ds(0, ROWS)], summed.at[pl.ds(ROWS * group_at, ROWS)],
            red_send.at[2], red_recv.at[2], device_id=in_group(step)[1], device_id_type=MESH,
        ).start()
    own = pltpu.make_async_copy(mid2.at[pl.ds(0, ROWS)], summed.at[pl.ds(ROWS * group_at, ROWS)], own_sem.at[2])
    own.start()
    own.wait()
    settle(send_sem, 0, xr, yr, xyr, zr)
    settle(send_sem, 1, xr2, yr2, xyr2, zr2)
    await_rows(red_send.at[0], got1, n_group - 1)
    await_rows(red_send.at[1], got2, n_line - 1)
    await_rows(red_recv.at[2], summed, n_group - 1)

    await_rows(red_send.at[2], summed, n_group - 1)


def finish(
    summed, gvol_v, gw1, gb1, gw2, gb2, gvol,
    gw1_v, gb1_v, gw2_v, gb2_v, sems,
):
    copies = [
        pltpu.make_async_copy(src, dst, sems.at[i])
        for i, (src, dst) in enumerate(((gvol_v, gvol), (gw2_v, gw2), (gw1_v, gw1), (gb1_v, gb1), (gb2_v, gb2)))
    ]
    copies[0].start()
    for k in range(4):
        block = summed[k * 16 : k * 16 + 16]
        for s in range(8):
            if k * 8 + s < 27:
                turned = pltpu.roll(block, (128 - 16 * s) % 128, 1) if s else block
                gw2_v[k * 8 + s] = turned[:, 0:16]
    copies[1].start()
    packed = summed[64:80].T
    for t in range(27):
        gw1_v[t] = packed[4 * t : 4 * t + 4, :]
    copies[2].start()
    gb1_v[...] = packed[108, :]
    gb2_v[...] = summed[48:64].T[48, :]
    copies[3].start()
    copies[4].start()
    for copy in copies:
        copy.wait()


def local(sizes, norm, volume, act_one, act_two, weight_one, weight_two, cotangent):
    narrow, wide, fold = constants()
    w1 = jnp.transpose(weight_one, (2, 3, 4, 1, 0)).reshape(27, CHAN_IN, CHAN)
    w2 = jnp.transpose(weight_two, (2, 3, 4, 0, 1)).reshape(27, CHAN, CHAN)
    n_group = sizes[0] * 4
    n_line = sizes[1] * (sizes[2] // 4)
    buf = lambda *shape: pltpu.VMEM(shape, BF16)
    buf32 = lambda *shape: pltpu.VMEM(shape, F32)
    block = (CHAN, NX, NY, NZ)
    summed, gvol = pl.pallas_call(
        functools.partial(kernel, sizes, norm),
        out_shape=(
            pltpu.VMEM((96, 128), F32),
            pltpu.VMEM((CHAN_IN, NX, NY, NZ), F32),
        ),
        in_specs=[pl.BlockSpec(memory_space=pl.ANY)] * 9,
        out_specs=tuple([pl.BlockSpec(memory_space=pltpu.VMEM)] * 2),
        scratch_shapes=[
            buf(CHAN_IN, NX, NY, NZ), buf(*block), buf(*block), buf(27, CHAN_IN, CHAN), buf(27, CHAN, CHAN), buf(*block),
            buf(NARROW, 128), buf(208, 512), buf(1152, 128),
            buf(2, 160, 128), buf(2, 160, 128), buf(2, 80, 128), buf(2, 80, 128), buf(4, 32, 128), buf32(2, 8, 128), buf32(2, 72, 128),
            buf(2, 128, 128), buf(2, 128, 128), buf(2, 64, 128), buf(2, 64, 128), buf(4, 16, 128), buf32(2, 8, 128), buf32(2, 72, 128),
            buf(4, 128, 128), buf(128, 512), buf(512, 768), buf32(128, 768), buf(3, 128, 512), buf(3, 32, 512),
            buf32(96, 128), buf32(4 * n_group, 128), buf32(4 * n_line, 128), buf32(8, 128), buf32(8, 128),
            pltpu.SemaphoreType.DMA((9,)), pltpu.SemaphoreType.DMA((3,)),
            pltpu.SemaphoreType.DMA((2, 4)), pltpu.SemaphoreType.DMA((2, 4)),
            pltpu.SemaphoreType.DMA((3,)), pltpu.SemaphoreType.DMA((3,)),
        ],
        compiler_params=pltpu.CompilerParams(collective_id=0, has_side_effects=True, vmem_limit_bytes=60 * 2**20),
        name="both_layers",
    )(volume, act_one, act_two, w1, w2, cotangent, narrow, wide, fold)
    shapes = ((27, CHAN_IN, CHAN), (CHAN,), (27, CHAN, CHAN), (CHAN,))
    gw1, gb1, gw2, gb2, gvol = pl.pallas_call(
        finish,
        out_shape=tuple(jax.ShapeDtypeStruct(shape, F32) for shape in shapes + ((CHAN_IN, NX, NY, NZ),)),
        in_specs=[pl.BlockSpec(memory_space=pltpu.VMEM)] * 2,
        out_specs=tuple([pl.BlockSpec(memory_space=pl.ANY)] * 5),
        scratch_shapes=[buf32(*shape) for shape in shapes] + [pltpu.SemaphoreType.DMA((5,))],
        compiler_params=pltpu.CompilerParams(vmem_limit_bytes=8 * 2**20),
        name="finish",
    )(summed, gvol)
    gw1 = jnp.transpose(gw1.reshape(3, 3, 3, CHAN_IN, CHAN), (4, 3, 0, 1, 2))
    gw2 = jnp.transpose(gw2.reshape(3, 3, 3, CHAN, CHAN), (3, 4, 0, 1, 2))
    return gw1, gb1, gw2, gb2, gvol


def solution(mesh):
    sizes = tuple(mesh.shape[name] for name in ("gx", "gy", "gz"))
    norm = 1.0 / math.sqrt(NX * NY * NZ * sizes[0] * sizes[1] * sizes[2])
    block = P(None, "gx", "gy", "gz")
    return jax.shard_map(
        functools.partial(local, sizes, norm),
        mesh=mesh,
        in_specs=(block, block, block, P(), P(), block),
        out_specs=(P(), P(), P(), P(), block),
        check_vma=False,
    )
```

```python
import functools
import math

import jax
import jax.numpy as jnp
import numpy as np
from jax import lax
from jax.experimental import pallas as pl
from jax.experimental.pallas import tpu as pltpu
from jax.sharding import PartitionSpec as P

CHAN_IN = 4
CHAN = 16
NX, NY, NZ = 4, 8, 128
F32, BF16 = jnp.float32, jnp.bfloat16
MESH = pl.DeviceIdType.MESH
ROWS = 3
SIDES = ((-1, 0), (1, 0), (0, -1), (0, 1), (-1, -1), (-1, 1), (1, -1), (1, 1))


def constants():
    r = np.arange(128)
    perm = np.zeros((128, 128), np.float32)
    perm[r, (r % 16) * 8 + r // 16] = 1
    eye = np.eye(128, dtype=np.float32)
    ends = np.zeros((16, 128), np.float32)
    ends[0, 0] = ends[1, 127] = 1
    tiles = np.zeros((32, 128), np.float32)
    for h in range(2):
        for x in range(4):
            for j in range(4):
                tiles[h * 16 + x * 4 + j, j * 32 + x * 8 + 7 * h] = 1
    rim_cols = np.zeros((48, 128), np.float32)
    rim_rows = np.zeros((48, 128), np.float32)
    for p in range(6):
        x = (p - 1) % 4
        for h in range(2):
            for j in range(4):
                rim_cols[p * 8 + h * 4 + j, j * 32 + x * 8 + 7 * (1 - h)] = 1
                tile = h if 1 <= p <= 4 else 2 + (0 if p == 0 else 2) + h
                rim_rows[p * 8 + h * 4 + j, tile * 16 + x * 4 + j] = 1
    spread = np.zeros((128, 128), np.float32)
    spread[r, r % 16] = 1
    narrow = np.concatenate([perm, eye, ends, tiles, rim_cols, rim_rows, spread])
    lane = np.arange(512)
    inside = lane < 480
    tap, end, chan = lane // 160, (lane % 160) // 16, lane % 16
    place = np.zeros((48, 512), np.float32)
    for c in range(3):
        for o in range(16):
            place[c * 16 + o] = inside & (tap == c) & (chan == o)
    y_two = (np.arange(128) // 16)[:, None]
    y_one = (np.arange(32) % 8)[:, None]
    band_two = np.where(inside[None], y_two + 2 - end[None], -9)
    band_one = np.where(inside[None], y_one + 2 - end[None], -9)
    wide = np.concatenate([place, band_two, band_one])
    rr = np.arange(128) % 40
    ok = np.arange(128) < 120
    row_y = np.where(rr < 32, 1 + rr % 8, np.where(rr < 36, 0, 9))
    row_j = np.where(rr < 32, rr // 8, rr % 4)
    row_c = np.arange(128) // 40
    y_of = np.broadcast_to(np.where(ok, row_y, -9)[None], (16, 128))
    fold = np.zeros((9, 128, 128), np.float32)
    for ab in range(9):
        for q in range(120):
            fold[ab, q, (ab * 3 + row_c[q]) * 4 + row_j[q]] = 1
    narrow = np.concatenate([narrow, y_of])
    return jnp.asarray(narrow, BF16), jnp.asarray(wide, BF16), jnp.asarray(fold.reshape(-1, 128), BF16)


AT = {}
_at = 0
for _name, _n in (("perm", 128), ("eye", 128), ("ends", 16), ("tiles", 32), ("rim_cols", 48), ("rim_rows", 48), ("spread", 128), ("y_of", 16)):
    AT[_name] = (_at, _n)
    _at += _n
NARROW = _at


def nt(a, b):
    return lax.dot_general(a, b, (((1,), (1,)), ((), ())), preferred_element_type=F32)


def nn(a, b):
    return jnp.dot(a, b, preferred_element_type=F32)


def way(dx, dy):
    return (dx + 1) * 3 + dy + 1


def corner(dx, dy):
    return (dx + 1) + (dy + 1) // 2


def kernel(
    sizes, norm,
    vol_h, act1_h, act2_h, w1_h, w2_h, cot_h, narrow_h, wide_h, fold_h,
    summed, gvol,
    vol_v, act1_v, act2_v, w1_v, w2_v, cot_v, narrow_v, wide_v, fold_v,
    xs, xr, ys, yr, xyr, zs, zr,
    xs2, xr2, ys2, yr2, xyr2, zs2, zr2,
    inner, acts, planes, rotated, volp, m_two, m_one, share, got1, got2, mid1, mid2,
    load_sem, own_sem, send_sem, recv_sem, red_send, red_recv,
):
    n_gx, n_gy, n_gz = sizes
    n_y = 4
    n_hi = n_gz // n_y
    n_group = n_gx * n_y
    n_line = n_gy * n_hi
    gx, gy, gz = lax.axis_index("gx"), lax.axis_index("gy"), lax.axis_index("gz")
    y_pos, hi_pos = lax.rem(gz, n_y), lax.div(gz, n_y)
    group_at = gx * n_y + y_pos
    line_at = hi_pos * n_gy + gy

    loads = [
        pltpu.make_async_copy(src, dst, load_sem.at[i])
        for i, (src, dst) in enumerate(
            ((cot_h, cot_v), (act2_h, act2_v), (narrow_h, narrow_v), (vol_h, vol_v), (act1_h, act1_v), (wide_h, wide_v), (w2_h, w2_v), (w1_h, w1_v), (fold_h, fold_v))
        )
    ]
    for copy in loads[:4]:
        copy.start()

    gx_at = [lax.rem(gx + d, n_gx) for d in range(n_gx)]
    gy_at = [lax.rem(gy + d, n_gy) for d in range(n_gy)]
    gz_at = [lax.rem(gz + d, n_gz) for d in range(n_gz)]
    y_at = [lax.rem(y_pos + d, n_y) for d in range(n_y)]
    line_to = [lax.rem(line_at + d, n_line) for d in range(n_line)]
    run_base = hi_pos * n_y

    def near(dx, dy, dz):
        return gx_at[dx], gy_at[dy], gz_at[dz]

    def ring(d, n):
        return min(d, n - d)

    group_steps = sorted(
        ((d, e) for d in range(n_gx) for e in range(n_y) if (d, e) != (0, 0)),
        key=lambda p: -(ring(p[0], n_gx) / 2 + ring(p[1], n_y)),
    )
    line_steps = sorted(range(1, n_line), key=lambda d: -ring(d, n_line))

    def in_group(step):
        d, e = step
        return gx_at[d] * n_y + y_at[e], (gx_at[d], gy, run_base + y_at[e])

    def in_line(d):
        return gx, lax.rem(line_to[d], n_gy), lax.div(line_to[d], n_gy) * n_y + y_pos

    barrier = pltpu.get_barrier_semaphore()
    for dz in (-1, 1, 0):
        for dx in (-1, 0, 1):
            for dy in (-1, 0, 1):
                if (dx, dy, dz) != (0, 0, 0):
                    pl.semaphore_signal(barrier, inc=1, device_id=near(dx, dy, dz), device_id_type=MESH)

    for d in line_steps:
        pl.semaphore_signal(barrier, inc=1, device_id=in_line(d), device_id_type=MESH)
    for step in group_steps:
        pl.semaphore_signal(barrier, inc=1, device_id=in_group(step)[1], device_id_type=MESH)
    for copy in loads[4:]:
        copy.start()

    def const(name):
        at, n = AT[name]
        return narrow_v[at : at + n, :]

    for i in range(4):
        loads[i].wait()
    perm, eye, ends = const("perm"), const("eye"), const("ends")

    def rows_of(ref, x):
        return ref[:, x].astype(F32).reshape(128, 128)

    def edge_rows(inner_at):
        return jnp.concatenate(
            [inner_at(x)[0:16] for x in range(4)] + [inner_at(x)[112:128] for x in range(4)], axis=0
        )

    row8 = lax.broadcasted_iota(jnp.int32, (8, 128), 0)

    def stack8(rows):
        out = jnp.zeros((8, 128), F32)
        for i, row in enumerate(rows):
            out = jnp.where(row8 == i, jnp.broadcast_to(row, (8, 128)), out)
        return out

    deltas = []
    for x in range(4):
        v = rows_of(cot_v, x)
        deltas.append(jnp.where(rows_of(act2_v, x) > 0, v, v * 0.3).astype(BF16))
    turned = nn(perm, jnp.concatenate(deltas, axis=1))
    bias_two = turned[:, 0:128] + turned[:, 128:256] + turned[:, 256:384] + turned[:, 384:512]
    turned = turned.astype(BF16)
    for x in range(4):
        inner[x] = turned[:, x * 128 : (x + 1) * 128]
    volflat = vol_v[...].astype(F32).reshape(128, 128).astype(BF16)
    vol_tiles = nn(const("tiles"), volflat).astype(BF16)

    def vol_rows(x):
        return vol_v[:, x].astype(F32).reshape(32, 128)

    xs[0, 0:128] = inner[0]
    xs[1, 0:128] = inner[3]
    xs[0, 128:160] = vol_rows(0).astype(BF16)
    xs[1, 128:160] = vol_rows(3).astype(BF16)
    for h in range(2):
        for at, x in ((0, 0), (2, 3), (3, 1), (4, 2)):
            ys[h, at * 16 : at * 16 + 16] = inner[x][112 * h : 112 * h + 16]
        ys[h, 16:32] = vol_tiles[16 * h : 16 * h + 16]
    z_face = nt(ends, jnp.concatenate([inner[x] for x in range(4)], axis=0))
    z_edge = nt(ends, edge_rows(lambda x: inner[x]))
    z_vol = nt(ends, volflat)
    for f in range(2):
        face = [z_face[f : f + 1, x * 128 : (x + 1) * 128] for x in range(4)]
        edge, flat = z_edge[f : f + 1], z_vol[f : f + 1]
        zs[f] = stack8([face[1], face[2], face[0], flat, face[3], edge, flat])

    pl.semaphore_wait(barrier, 26 + (n_line - 1) + (n_group - 1))

    def exchange(phase, xs, xr, ys, yr, xyr, zs, zr):
        first = phase == 0
        out = []

        def send(kind, src, dst, where):
            copy = pltpu.make_async_remote_copy(
                src, dst, send_sem.at[phase, kind], recv_sem.at[phase, kind], device_id=where, device_id_type=MESH
            )
            copy.start()
            out.append(copy)

        for dz in (-1, 1):
            f, side = (1 if dz == 1 else 0), (0 if dz == 1 else 1)
            for dx in (-1, 0, 1):
                for dy in (-1, 0, 1):
                    if first:
                        at, n = {-1: (2, 2), 1: (3, 2), 0: (0, 5) if dy == 0 else (5, 2)}[dx]
                    else:
                        at, n = {-1: (2, 1), 1: (3, 1), 0: (0, 4) if dy == 0 else (4, 1)}[dx]
                    send(0, zs.at[f, pl.ds(at, n)], zr.at[side, pl.ds(8 * way(-dx, -dy), n)], near(dx, dy, dz))
        for dx in (-1, 1):
            send(1, xs.at[(dx + 1) // 2], xr.at[(1 - dx) // 2], near(dx, 0, 0))
        for dy in (-1, 1):
            send(2, ys.at[(dy + 1) // 2], yr.at[(1 - dy) // 2], near(0, dy, 0))
        for dx in (-1, 1):
            for dy in (-1, 1):
                if first:
                    at, n = (0 if dx == -1 else 16), 32
                else:
                    at, n = (0 if dx == -1 else 16), 16
                send(3, ys.at[(dy + 1) // 2, pl.ds(at, n)], xyr.at[corner(-dx, -dy)], near(dx, dy, 0))

    def settle(sems, phase, kinds, xr, yr, xyr, zr):
        refs = (zr.at[0, pl.ds(0, 42 if phase == 0 else 24)], xr, yr, xyr)
        for kind in kinds:
            pltpu.make_async_copy(refs[kind], refs[kind], sems.at[phase, kind]).wait()

    lane_of = lax.broadcasted_iota(jnp.int32, (160, 128), 1)

    TURNS = ((0, 1, 127, 127), (2, 0, 1, 0))

    def build_planes(phase, inner_at, xr, yr, xyr):
        first = phase == 0
        tile_at = {0: 0, 3: 2, 1: 3, 2: 4} if first else {0: 0, 3: 1, 1: 2, 2: 3}
        for p in range(6):
            if 1 <= p <= 4:
                x = p - 1
                low = yr[0, tile_at[x] * 16 : tile_at[x] * 16 + 16]
                mid = inner_at(x)
                high = yr[1, tile_at[x] * 16 : tile_at[x] * 16 + 16]
            else:
                dx = -1 if p == 0 else 1
                at = (16 if dx == -1 else 0) if first else 0
                low = xyr[corner(dx, -1), at : at + 16]
                mid = xr[(dx + 1) // 2, 0:128]
                high = xyr[corner(dx, 1), at : at + 16]
            plane = jnp.concatenate([low, mid, high], axis=0)
            lanes = slice(p * 128, (p + 1) * 128)
            planes[160:320, lanes] = plane
            plane = plane.astype(F32)
            for tap, side, turn, lane in TURNS:
                rotated[side, :, lanes] = pltpu.roll(plane, turn, 1)

    def close_planes(phase, zr):
        first = phase == 0
        cols = nt(eye, zr[...].reshape(144, 128).astype(BF16))
        face_at = {0: 2, 3: 4, 1: 0, 2: 1} if first else {0: 2, 3: 3, 1: 0, 2: 1}
        for p in range(6):
            if 1 <= p <= 4:
                x = p - 1
                pick = (
                    (64 + 16 * x, 80 + 16 * x, 8 * way(0, -1)),
                    (0, 128, 8 * way(0, 0) + face_at[x]),
                    (16 * x, 16 * x + 16, 8 * way(0, 1)),
                )
            else:
                dx = -1 if p == 0 else 1
                r = (1 if dx == -1 else 0) if first else 0
                pick = (
                    (112, 128, 8 * way(dx, -1) + r),
                    (0, 128, 8 * way(dx, 0) + r),
                    (0, 16, 8 * way(dx, 1) + r),
                )
            lanes = slice(p * 128, (p + 1) * 128)
            for tap, side, turn, lane in TURNS:
                col = jnp.concatenate(
                    [cols[a:b, 72 * side + k : 72 * side + k + 1] for a, b, k in pick], axis=0
                )
                shifted = jnp.where(lane_of == lane, jnp.broadcast_to(col, (160, 128)), rotated[side, :, lanes])
                planes[tap * 160 : tap * 160 + 160, lanes] = shifted.astype(BF16)
        return cols

    exchange(0, xs, xr, ys, yr, xyr, zs, zr)

    for i in range(4, 9):
        loads[i].wait()
    turned = nn(perm, jnp.concatenate([rows_of(act1_v, x).astype(BF16) for x in range(4)], axis=1))
    acts[...] = turned.astype(BF16)
    planes[480:512, :] = jnp.zeros((32, 768), BF16)
    place = wide_v[0:48, :]
    band_two = wide_v[48:176, :].astype(F32)
    band_one = wide_v[176:208, :].astype(F32)
    spread = const("spread")[:, 0:16]
    for a in range(3):
        total_two = jnp.zeros((128, 512), F32)
        total_one = jnp.zeros((32, 512), F32)
        for b in range(3):
            t = (a * 3 + b) * 3
            group = w2_v[t : t + 3].reshape(48, 16)
            wide = nn(nt(spread, group).astype(BF16), place)
            total_two = jnp.where(band_two == b, wide, total_two)
            four = jnp.zeros((4, 512), F32)
            for c in range(3):
                four = four + nn(w1_v[t + c], place[c * 16 : c * 16 + 16])
            wide = jnp.concatenate([jnp.broadcast_to(four[j : j + 1], (8, 512)) for j in range(4)], axis=0)
            total_one = jnp.where(band_one == b, wide, total_one)
        m_two[a] = total_two.astype(BF16)
        m_one[a] = total_one.astype(BF16)

    settle(recv_sem, 0, (1, 2, 3), xr, yr, xyr, zr)
    build_planes(0, lambda x: inner[x], xr, yr, xyr)

    v_tiles = jnp.concatenate(
        [yr[0, 16:32], yr[1, 16:32]]
        + [xyr[corner(dx, dy), at : at + 16] for dx, at in ((-1, 0), (1, 16)) for dy in (-1, 1)],
        axis=0,
    )
    rims = nn(const("rim_rows")[:, 0:96], v_tiles)
    volp[120:128, :] = jnp.zeros((8, 768), F32)
    for p in range(6):
        mid = vol_rows(p - 1) if 1 <= p <= 4 else xr[p // 5, 128:160].astype(F32)
        plane = jnp.concatenate([mid, rims[p * 8 : p * 8 + 8]], axis=0)
        lanes = slice(p * 128, (p + 1) * 128)
        volp[40:80, lanes] = plane
        volp[0:40, lanes] = pltpu.roll(plane, 1, 1)
        volp[80:120, lanes] = pltpu.roll(plane, 127, 1)

    settle(recv_sem, 0, (0,), xr, yr, xyr, zr)
    cols = close_planes(0, zr)

    back = nn(m_two[0], planes[:, 256:768]) + nn(m_two[1], planes[:, 128:640]) + nn(m_two[2], planes[:, 0:512])
    delta = jnp.where(acts[...].astype(F32) > 0, back, back * 0.3).astype(BF16)
    wide_delta = delta.astype(F32)
    bias_one = wide_delta[:, 0:128] + wide_delta[:, 128:256] + wide_delta[:, 256:384] + wide_delta[:, 384:512]

    def delta_at(x):
        return delta[:, x * 128 : (x + 1) * 128]

    rim_cols = nn(const("rim_cols"), cols.astype(BF16))
    lane40 = lax.broadcasted_iota(jnp.int32, (40, 128), 1)
    half8 = lax.broadcasted_iota(jnp.int32, (8, 1), 0) < 4
    for p in range(6):
        x = (p - 1) % 4
        dx = -1 if p == 0 else (1 if p == 5 else 0)
        lanes = slice(p * 128, (p + 1) * 128)
        r = {-1: 0, 1: 1, 0: 1}[dx]
        for tap, side, lane in ((0, 0, 0), (2, 1, 127)):
            k = 72 * side + 8 * way(dx, 0) + (3 if dx == 0 else r)
            low, high = (72 * side + 8 * way(dx, e) + r for e in (-1, 1))
            col = jnp.concatenate(
                [cols[j * 32 + x * 8 : j * 32 + x * 8 + 8, k : k + 1] for j in range(4)]
                + [
                    jnp.where(
                        half8,
                        rim_cols[p * 8 : p * 8 + 8, low : low + 1],
                        rim_cols[p * 8 : p * 8 + 8, high : high + 1],
                    )
                ],
                axis=0,
            )
            rows = slice(tap * 40, tap * 40 + 40)
            volp[rows, lanes] = jnp.where(lane40 == lane, jnp.broadcast_to(col, (40, 128)), volp[rows, lanes])

    y_of = const("y_of").astype(F32)
    sums = []
    for a in range(3):
        g = nt(delta, volp[:, a * 128 : (a + 4) * 128].astype(BF16))
        for b in range(3):
            total = jnp.zeros((16, 128), F32)
            for y in range(8):
                total = total + jnp.where(y_of == y + b, g[y * 16 : y * 16 + 16], 0.0)
            sums.append(total)
    sums = jnp.concatenate(sums, axis=1)
    top = sums.astype(BF16)
    rest = (sums - top.astype(F32)).astype(BF16)
    fold = fold_v[...]
    packed = nn(top, fold) + nn(rest, fold)

    def fold_y(v):
        out = v[0:16]
        for y in range(1, 8):
            out = out + v[y * 16 : y * 16 + 16]
        return jnp.broadcast_to(jnp.sum(out, axis=1, keepdims=True), (16, 128))

    lane16 = lax.broadcasted_iota(jnp.int32, (16, 128), 1)
    share[64:80] = jnp.where(lane16 >= 108, fold_y(bias_one), packed)
    share[80:96] = jnp.zeros((16, 128), F32)

    slot = lax.shift_right_logical(lane16, 4)
    blocks = [jnp.zeros((16, 128), F32) for _ in range(4)]
    for a in range(3):
        g = nt(planes[0:480, (2 - a) * 128 : (6 - a) * 128], acts[...])
        for b in range(3):
            for c in range(3):
                t = (a * 3 + b) * 3 + c
                total = jnp.zeros((16, 128), F32)
                for y in range(8):
                    at = c * 160 + (y + 2 - b) * 16
                    total = jnp.where(slot == y, g[at : at + 16], total)
                for turn in (64, 32, 16):
                    total = total + pltpu.roll(total, turn, 1)
                blocks[t // 8] = jnp.where(slot == t % 8, total, blocks[t // 8])
    blocks[3] = jnp.where(slot == 3, fold_y(bias_two), blocks[3])
    for k in range(4):
        share[k * 16 : k * 16 + 16] = blocks[k]

    for step in group_steps:
        t, where = in_group(step)
        pltpu.make_async_remote_copy(
            share.at[pl.ds(ROWS * t, ROWS)], got1.at[pl.ds(4 * group_at, ROWS)],
            red_send.at[0], red_recv.at[0], device_id=where, device_id_type=MESH,
        ).start()
    own = pltpu.make_async_copy(share.at[pl.ds(ROWS * group_at, ROWS)], got1.at[pl.ds(4 * group_at, ROWS)], own_sem.at[0])
    own.start()
    own.wait()

    xs2[0] = delta_at(0)
    xs2[1] = delta_at(3)
    for h in range(2):
        for at, x in ((0, 0), (1, 3), (2, 1), (3, 2)):
            ys2[h, at * 16 : at * 16 + 16] = delta_at(x)[112 * h : 112 * h + 16]
    z_face = nt(ends, jnp.concatenate([delta_at(x) for x in range(4)], axis=0))
    z_edge = nt(ends, edge_rows(delta_at))
    for f in range(2):
        face = [z_face[f : f + 1, x * 128 : (x + 1) * 128] for x in range(4)]
        zs2[f] = stack8([face[1], face[2], face[0], face[3], z_edge[f : f + 1]])
    exchange(1, xs2, xr2, ys2, yr2, xyr2, zs2, zr2)
    for x in range(4):
        inner[x] = delta_at(x)

    def await_rows(sem, ref, n):
        ref = ref.at[pl.ds(0, n * ROWS)]
        pltpu.make_async_copy(ref, ref, sem).wait()

    def total8(ref, n):
        out = ref[0:8]
        for i in range(1, n // 2):
            out = out + ref[i * 8 : i * 8 + 8]
        return out + pltpu.roll(out, 4, 0)

    await_rows(red_recv.at[0], got1, n_group - 1)
    mid1[...] = total8(got1, n_group)

    for d in line_steps:
        pltpu.make_async_remote_copy(
            mid1.at[pl.ds(0, ROWS)], got2.at[pl.ds(4 * line_at, ROWS)],
            red_send.at[1], red_recv.at[1], device_id=in_line(d), device_id_type=MESH,
        ).start()
    own = pltpu.make_async_copy(mid1.at[pl.ds(0, ROWS)], got2.at[pl.ds(4 * line_at, ROWS)], own_sem.at[1])
    own.start()
    own.wait()

    await_rows(red_recv.at[1], got2, n_line - 1)
    mid2[...] = total8(got2, n_line) * norm

    for step in group_steps:
        pltpu.make_async_remote_copy(
            mid2.at[pl.ds(0, ROWS)], summed.at[pl.ds(ROWS * group_at, ROWS)],
            red_send.at[2], red_recv.at[2], device_id=in_group(step)[1], device_id_type=MESH,
        ).start()
    own = pltpu.make_async_copy(mid2.at[pl.ds(0, ROWS)], summed.at[pl.ds(ROWS * group_at, ROWS)], own_sem.at[2])
    own.start()
    own.wait()
    settle(recv_sem, 1, range(4), xr2, yr2, xyr2, zr2)
    build_planes(1, lambda x: inner[x], xr2, yr2, xyr2)
    close_planes(1, zr2)
    grad = nn(m_one[0], planes[:, 256:768]) + nn(m_one[1], planes[:, 128:640]) + nn(m_one[2], planes[:, 0:512])
    for j in range(4):
        for x in range(4):
            gvol[j, x] = grad[j * 8 : j * 8 + 8, x * 128 : (x + 1) * 128]

    settle(send_sem, 0, range(4), xr, yr, xyr, zr)
    settle(send_sem, 1, range(4), xr2, yr2, xyr2, zr2)
    await_rows(red_send.at[0], got1, n_group - 1)
    await_rows(red_send.at[1], got2, n_line - 1)
    await_rows(red_recv.at[2], summed, n_group - 1)

    await_rows(red_send.at[2], summed, n_group - 1)


def finish(
    summed, gvol_v, gw1, gb1, gw2, gb2, gvol,
    gw1_v, gb1_v, gw2_v, gb2_v, sems,
):
    copies = [
        pltpu.make_async_copy(src, dst, sems.at[i])
        for i, (src, dst) in enumerate(((gvol_v, gvol), (gw2_v, gw2), (gw1_v, gw1), (gb1_v, gb1), (gb2_v, gb2)))
    ]
    copies[0].start()
    for k in range(4):
        block = summed[k * 16 : k * 16 + 16]
        for s in range(8):
            if k * 8 + s < 27:
                turned = pltpu.roll(block, (128 - 16 * s) % 128, 1) if s else block
                gw2_v[k * 8 + s] = turned[:, 0:16]
    copies[1].start()
    packed = summed[64:80].T
    for t in range(27):
        gw1_v[t] = packed[4 * t : 4 * t + 4, :]
    copies[2].start()
    gb1_v[...] = packed[108, :]
    gb2_v[...] = summed[48:64].T[48, :]
    copies[3].start()
    copies[4].start()
    for copy in copies:
        copy.wait()


def local(sizes, norm, volume, act_one, act_two, weight_one, weight_two, cotangent):
    narrow, wide, fold = constants()
    w1 = jnp.transpose(weight_one, (2, 3, 4, 1, 0)).reshape(27, CHAN_IN, CHAN)
    w2 = jnp.transpose(weight_two, (2, 3, 4, 0, 1)).reshape(27, CHAN, CHAN)
    n_group = sizes[0] * 4
    n_line = sizes[1] * (sizes[2] // 4)
    buf = lambda *shape: pltpu.VMEM(shape, BF16)
    buf32 = lambda *shape: pltpu.VMEM(shape, F32)
    block = (CHAN, NX, NY, NZ)
    summed, gvol = pl.pallas_call(
        functools.partial(kernel, sizes, norm),
        out_shape=(
            pltpu.VMEM((96, 128), F32),
            pltpu.VMEM((CHAN_IN, NX, NY, NZ), F32),
        ),
        in_specs=[pl.BlockSpec(memory_space=pl.ANY)] * 9,
        out_specs=tuple([pl.BlockSpec(memory_space=pltpu.VMEM)] * 2),
        scratch_shapes=[
            buf(CHAN_IN, NX, NY, NZ), buf(*block), buf(*block), buf(27, CHAN_IN, CHAN), buf(27, CHAN, CHAN), buf(*block),
            buf(NARROW, 128), buf(208, 512), buf(1152, 128),
            buf(2, 160, 128), buf(2, 160, 128), buf(2, 80, 128), buf(2, 80, 128), buf(4, 32, 128), buf32(2, 8, 128), buf32(2, 72, 128),
            buf(2, 128, 128), buf(2, 128, 128), buf(2, 64, 128), buf(2, 64, 128), buf(4, 16, 128), buf32(2, 8, 128), buf32(2, 72, 128),
            buf(4, 128, 128), buf(128, 512), buf(512, 768), buf32(2, 160, 768), buf32(128, 768), buf(3, 128, 512), buf(3, 32, 512),
            buf32(96, 128), buf32(4 * n_group, 128), buf32(4 * n_line, 128), buf32(8, 128), buf32(8, 128),
            pltpu.SemaphoreType.DMA((9,)), pltpu.SemaphoreType.DMA((3,)),
            pltpu.SemaphoreType.DMA((2, 4)), pltpu.SemaphoreType.DMA((2, 4)),
            pltpu.SemaphoreType.DMA((3,)), pltpu.SemaphoreType.DMA((3,)),
        ],
        compiler_params=pltpu.CompilerParams(collective_id=0, has_side_effects=True, vmem_limit_bytes=60 * 2**20),
        name="both_layers",
    )(volume, act_one, act_two, w1, w2, cotangent, narrow, wide, fold)
    shapes = ((27, CHAN_IN, CHAN), (CHAN,), (27, CHAN, CHAN), (CHAN,))
    gw1, gb1, gw2, gb2, gvol = pl.pallas_call(
        finish,
        out_shape=tuple(jax.ShapeDtypeStruct(shape, F32) for shape in shapes + ((CHAN_IN, NX, NY, NZ),)),
        in_specs=[pl.BlockSpec(memory_space=pltpu.VMEM)] * 2,
        out_specs=tuple([pl.BlockSpec(memory_space=pl.ANY)] * 5),
        scratch_shapes=[buf32(*shape) for shape in shapes] + [pltpu.SemaphoreType.DMA((5,))],
        compiler_params=pltpu.CompilerParams(vmem_limit_bytes=8 * 2**20),
        name="finish",
    )(summed, gvol)
    gw1 = jnp.transpose(gw1.reshape(3, 3, 3, CHAN_IN, CHAN), (4, 3, 0, 1, 2))
    gw2 = jnp.transpose(gw2.reshape(3, 3, 3, CHAN, CHAN), (3, 4, 0, 1, 2))
    return gw1, gb1, gw2, gb2, gvol


def solution(mesh):
    sizes = tuple(mesh.shape[name] for name in ("gx", "gy", "gz"))
    norm = 1.0 / math.sqrt(NX * NY * NZ * sizes[0] * sizes[1] * sizes[2])
    block = P(None, "gx", "gy", "gz")
    return jax.shard_map(
        functools.partial(local, sizes, norm),
        mesh=mesh,
        in_specs=(block, block, block, P(), P(), block),
        out_specs=(P(), P(), P(), P(), block),
        check_vma=False,
    )
```

```python
import functools
import math

import jax
import jax.numpy as jnp
import numpy as np
from jax import lax
from jax.experimental import pallas as pl
from jax.experimental.pallas import tpu as pltpu
from jax.sharding import PartitionSpec as P

CHAN_IN = 4
CHAN = 16
NX, NY, NZ = 4, 8, 128
F32, BF16 = jnp.float32, jnp.bfloat16
MESH = pl.DeviceIdType.MESH
ROWS = 3
SIDES = ((-1, 0), (1, 0), (0, -1), (0, 1), (-1, -1), (-1, 1), (1, -1), (1, 1))


def constants():
    r = np.arange(128)
    perm = np.zeros((128, 128), np.float32)
    perm[r, (r % 16) * 8 + r // 16] = 1
    eye = np.eye(128, dtype=np.float32)
    ends = np.zeros((16, 128), np.float32)
    ends[0, 0] = ends[1, 127] = 1
    tiles = np.zeros((32, 128), np.float32)
    for h in range(2):
        for x in range(4):
            for j in range(4):
                tiles[h * 16 + x * 4 + j, j * 32 + x * 8 + 7 * h] = 1
    rim_cols = np.zeros((48, 128), np.float32)
    rim_rows = np.zeros((48, 128), np.float32)
    for p in range(6):
        x = (p - 1) % 4
        for h in range(2):
            for j in range(4):
                rim_cols[p * 8 + h * 4 + j, j * 32 + x * 8 + 7 * (1 - h)] = 1
                tile = h if 1 <= p <= 4 else 2 + (0 if p == 0 else 2) + h
                rim_rows[p * 8 + h * 4 + j, tile * 16 + x * 4 + j] = 1
    spread = np.zeros((128, 128), np.float32)
    spread[r, r % 16] = 1
    narrow = np.concatenate([perm, eye, ends, tiles, rim_cols, rim_rows, spread])
    lane = np.arange(512)
    inside = lane < 480
    tap, end, chan = lane // 160, (lane % 160) // 16, lane % 16
    place = np.zeros((48, 512), np.float32)
    for c in range(3):
        for o in range(16):
            place[c * 16 + o] = inside & (tap == c) & (chan == o)
    y_two = (np.arange(128) // 16)[:, None]
    y_one = (np.arange(32) % 8)[:, None]
    band_two = np.where(inside[None], y_two + 2 - end[None], -9)
    band_one = np.where(inside[None], y_one + 2 - end[None], -9)
    wide = np.concatenate([place, band_two, band_one])
    rr = np.arange(128) % 40
    ok = np.arange(128) < 120
    row_y = np.where(rr < 32, 1 + rr % 8, np.where(rr < 36, 0, 9))
    row_j = np.where(rr < 32, rr // 8, rr % 4)
    row_c = np.arange(128) // 40
    y_of = np.broadcast_to(np.where(ok, row_y, -9)[None], (16, 128))
    fold = np.zeros((9, 128, 128), np.float32)
    for ab in range(9):
        for q in range(120):
            fold[ab, q, (ab * 3 + row_c[q]) * 4 + row_j[q]] = 1
    narrow = np.concatenate([narrow, y_of])
    return jnp.asarray(narrow, BF16), jnp.asarray(wide, BF16), jnp.asarray(fold.reshape(-1, 128), BF16)


AT = {}
_at = 0
for _name, _n in (("perm", 128), ("eye", 128), ("ends", 16), ("tiles", 32), ("rim_cols", 48), ("rim_rows", 48), ("spread", 128), ("y_of", 16)):
    AT[_name] = (_at, _n)
    _at += _n
NARROW = _at


def nt(a, b):
    return lax.dot_general(a, b, (((1,), (1,)), ((), ())), preferred_element_type=F32)


def nn(a, b):
    return jnp.dot(a, b, preferred_element_type=F32)


def way(dx, dy):
    return (dx + 1) * 3 + dy + 1


def corner(dx, dy):
    return (dx + 1) + (dy + 1) // 2


def kernel(
    sizes, norm,
    vol_h, act1_h, act2_h, w1_h, w2_h, cot_h, narrow_h, wide_h, fold_h,
    summed, gvol,
    vol_v, act1_v, act2_v, w1_v, w2_v, cot_v, narrow_v, wide_v, fold_v,
    xs, xr, ys, yr, xyr, zs, zr,
    xs2, xr2, ys2, yr2, xyr2, zs2, zr2,
    inner, acts, planes, rotated, volp, m_two, m_one, share, got1, got2, mid1, mid2,
    load_sem, own_sem, send_sem, recv_sem, red_send, red_recv,
):
    n_gx, n_gy, n_gz = sizes
    n_y = 4
    n_hi = n_gz // n_y
    n_group = n_gx * n_y
    n_line = n_gy * n_hi
    gx, gy, gz = lax.axis_index("gx"), lax.axis_index("gy"), lax.axis_index("gz")
    y_pos, hi_pos = lax.rem(gz, n_y), lax.div(gz, n_y)
    group_at = gx * n_y + y_pos
    line_at = hi_pos * n_gy + gy

    loads = [
        pltpu.make_async_copy(src, dst, load_sem.at[i])
        for i, (src, dst) in enumerate(
            ((cot_h, cot_v), (act2_h, act2_v), (narrow_h, narrow_v), (vol_h, vol_v), (act1_h, act1_v), (wide_h, wide_v), (w2_h, w2_v), (w1_h, w1_v), (fold_h, fold_v))
        )
    ]
    for copy in loads[:4]:
        copy.start()

    gx_at = [lax.rem(gx + d, n_gx) for d in range(n_gx)]
    gy_at = [lax.rem(gy + d, n_gy) for d in range(n_gy)]
    gz_at = [lax.rem(gz + d, n_gz) for d in range(n_gz)]
    y_at = [lax.rem(y_pos + d, n_y) for d in range(n_y)]
    line_to = [lax.rem(line_at + d, n_line) for d in range(n_line)]
    run_base = hi_pos * n_y

    def near(dx, dy, dz):
        return gx_at[dx], gy_at[dy], gz_at[dz]

    def ring(d, n):
        return min(d, n - d)

    group_steps = sorted(
        ((d, e) for d in range(n_gx) for e in range(n_y) if (d, e) != (0, 0)),
        key=lambda p: -(ring(p[0], n_gx) / 2 + ring(p[1], n_y)),
    )
    line_steps = sorted(range(1, n_line), key=lambda d: -ring(d, n_line))

    def in_group(step):
        d, e = step
        return gx_at[d] * n_y + y_at[e], (gx_at[d], gy, run_base + y_at[e])

    def in_line(d):
        return gx, lax.rem(line_to[d], n_gy), lax.div(line_to[d], n_gy) * n_y + y_pos

    barrier = pltpu.get_barrier_semaphore()
    for dz in (-1, 1, 0):
        for dx in (-1, 0, 1):
            for dy in (-1, 0, 1):
                if (dx, dy, dz) != (0, 0, 0):
                    pl.semaphore_signal(barrier, inc=1, device_id=near(dx, dy, dz), device_id_type=MESH)

    for d in line_steps:
        pl.semaphore_signal(barrier, inc=1, device_id=in_line(d), device_id_type=MESH)
    for step in group_steps:
        pl.semaphore_signal(barrier, inc=1, device_id=in_group(step)[1], device_id_type=MESH)
    for copy in loads[4:]:
        copy.start()

    def const(name):
        at, n = AT[name]
        return narrow_v[at : at + n, :]

    for i in range(4):
        loads[i].wait()
    perm, eye, ends = const("perm"), const("eye"), const("ends")

    def rows_of(ref, x):
        return ref[:, x].astype(F32).reshape(128, 128)

    def edge_rows(inner_at):
        return jnp.concatenate(
            [inner_at(x)[0:16] for x in range(4)] + [inner_at(x)[112:128] for x in range(4)], axis=0
        )

    row8 = lax.broadcasted_iota(jnp.int32, (8, 128), 0)

    def stack8(rows):
        out = jnp.zeros((8, 128), F32)
        for i, row in enumerate(rows):
            out = jnp.where(row8 == i, jnp.broadcast_to(row, (8, 128)), out)
        return out

    deltas = []
    for x in range(4):
        v = rows_of(cot_v, x)
        deltas.append(jnp.where(rows_of(act2_v, x) > 0, v, v * 0.3).astype(BF16))
    turned = nn(perm, jnp.concatenate(deltas, axis=1))
    bias_two = turned[:, 0:128] + turned[:, 128:256] + turned[:, 256:384] + turned[:, 384:512]
    turned = turned.astype(BF16)
    for x in range(4):
        inner[x] = turned[:, x * 128 : (x + 1) * 128]
    volflat = vol_v[...].astype(F32).reshape(128, 128).astype(BF16)
    vol_tiles = nn(const("tiles"), volflat).astype(BF16)

    def vol_rows(x):
        return vol_v[:, x].astype(F32).reshape(32, 128)

    xs[0, 0:128] = inner[0]
    xs[1, 0:128] = inner[3]
    xs[0, 128:160] = vol_rows(0).astype(BF16)
    xs[1, 128:160] = vol_rows(3).astype(BF16)
    for h in range(2):
        for at, x in ((0, 0), (2, 3), (3, 1), (4, 2)):
            ys[h, at * 16 : at * 16 + 16] = inner[x][112 * h : 112 * h + 16]
        ys[h, 16:32] = vol_tiles[16 * h : 16 * h + 16]
    z_face = nt(ends, jnp.concatenate([inner[x] for x in range(4)], axis=0))
    z_edge = nt(ends, edge_rows(lambda x: inner[x]))
    z_vol = nt(ends, volflat)
    for f in range(2):
        face = [z_face[f : f + 1, x * 128 : (x + 1) * 128] for x in range(4)]
        edge, flat = z_edge[f : f + 1], z_vol[f : f + 1]
        zs[f] = stack8([face[1], face[2], face[0], flat, face[3], edge, flat])

    pl.semaphore_wait(barrier, 26 + (n_line - 1) + (n_group - 1))

    def exchange(phase, xs, xr, ys, yr, xyr, zs, zr):
        first = phase == 0
        out = []

        def send(kind, src, dst, where):
            copy = pltpu.make_async_remote_copy(
                src, dst, send_sem.at[phase, kind], recv_sem.at[phase, kind], device_id=where, device_id_type=MESH
            )
            copy.start()
            out.append(copy)

        for dz in (-1, 1):
            f, side = (1 if dz == 1 else 0), (0 if dz == 1 else 1)
            for dx in (-1, 0, 1):
                for dy in (-1, 0, 1):
                    if first:
                        at, n = {-1: (2, 2), 1: (3, 2), 0: (0, 5) if dy == 0 else (5, 2)}[dx]
                    else:
                        at, n = {-1: (2, 1), 1: (3, 1), 0: (0, 4) if dy == 0 else (4, 1)}[dx]
                    send(0, zs.at[f, pl.ds(at, n)], zr.at[side, pl.ds(8 * way(-dx, -dy), n)], near(dx, dy, dz))
        for dx in (-1, 1):
            send(1, xs.at[(dx + 1) // 2], xr.at[(1 - dx) // 2], near(dx, 0, 0))
        for dy in (-1, 1):
            send(2, ys.at[(dy + 1) // 2], yr.at[(1 - dy) // 2], near(0, dy, 0))
        for dx in (-1, 1):
            for dy in (-1, 1):
                if first:
                    at, n = (0 if dx == -1 else 16), 32
                else:
                    at, n = (0 if dx == -1 else 16), 16
                send(3, ys.at[(dy + 1) // 2, pl.ds(at, n)], xyr.at[corner(-dx, -dy)], near(dx, dy, 0))

    def settle(sems, phase, kinds, xr, yr, xyr, zr):
        refs = (zr.at[0, pl.ds(0, 42 if phase == 0 else 24)], xr, yr, xyr)
        for kind in kinds:
            pltpu.make_async_copy(refs[kind], refs[kind], sems.at[phase, kind]).wait()

    lane_of = lax.broadcasted_iota(jnp.int32, (160, 128), 1)

    TURNS = ((0, 1, 127, 127), (2, 0, 1, 0))

    def build_planes(phase, inner_at, xr, yr, xyr):
        first = phase == 0
        tile_at = {0: 0, 3: 2, 1: 3, 2: 4} if first else {0: 0, 3: 1, 1: 2, 2: 3}
        for p in range(6):
            if 1 <= p <= 4:
                x = p - 1
                low = yr[0, tile_at[x] * 16 : tile_at[x] * 16 + 16]
                mid = inner_at(x)
                high = yr[1, tile_at[x] * 16 : tile_at[x] * 16 + 16]
            else:
                dx = -1 if p == 0 else 1
                at = (16 if dx == -1 else 0) if first else 0
                low = xyr[corner(dx, -1), at : at + 16]
                mid = xr[(dx + 1) // 2, 0:128]
                high = xyr[corner(dx, 1), at : at + 16]
            plane = jnp.concatenate([low, mid, high], axis=0)
            lanes = slice(p * 128, (p + 1) * 128)
            planes[160:320, lanes] = plane
            plane = plane.astype(F32)
            for tap, side, turn, lane in TURNS:
                rotated[side, :, lanes] = pltpu.roll(plane, turn, 1)

    def close_planes(phase, zr):
        first = phase == 0
        cols = nt(eye, zr[...].reshape(144, 128).astype(BF16))
        face_at = {0: 2, 3: 4, 1: 0, 2: 1} if first else {0: 2, 3: 3, 1: 0, 2: 1}
        for p in range(6):
            if 1 <= p <= 4:
                x = p - 1
                pick = (
                    (64 + 16 * x, 80 + 16 * x, 8 * way(0, -1)),
                    (0, 128, 8 * way(0, 0) + face_at[x]),
                    (16 * x, 16 * x + 16, 8 * way(0, 1)),
                )
            else:
                dx = -1 if p == 0 else 1
                r = (1 if dx == -1 else 0) if first else 0
                pick = (
                    (112, 128, 8 * way(dx, -1) + r),
                    (0, 128, 8 * way(dx, 0) + r),
                    (0, 16, 8 * way(dx, 1) + r),
                )
            lanes = slice(p * 128, (p + 1) * 128)
            for tap, side, turn, lane in TURNS:
                col = jnp.concatenate(
                    [cols[a:b, 72 * side + k : 72 * side + k + 1] for a, b, k in pick], axis=0
                )
                shifted = jnp.where(lane_of == lane, jnp.broadcast_to(col, (160, 128)), rotated[side, :, lanes])
                planes[tap * 160 : tap * 160 + 160, lanes] = shifted.astype(BF16)
        return cols

    exchange(0, xs, xr, ys, yr, xyr, zs, zr)

    for i in range(4, 9):
        loads[i].wait()
    turned = nn(perm, jnp.concatenate([rows_of(act1_v, x).astype(BF16) for x in range(4)], axis=1))
    acts[...] = turned.astype(BF16)
    planes[480:512, :] = jnp.zeros((32, 768), BF16)
    place = wide_v[0:48, :]
    band_two = wide_v[48:176, :].astype(F32)
    band_one = wide_v[176:208, :].astype(F32)
    spread = const("spread")[:, 0:16]
    for a in range(3):
        total_two = jnp.zeros((128, 512), F32)
        total_one = jnp.zeros((32, 512), F32)
        for b in range(3):
            t = (a * 3 + b) * 3
            group = w2_v[t : t + 3].reshape(48, 16)
            wide = nn(nt(spread, group).astype(BF16), place)
            total_two = jnp.where(band_two == b, wide, total_two)
            four = jnp.zeros((4, 512), F32)
            for c in range(3):
                four = four + nn(w1_v[t + c], place[c * 16 : c * 16 + 16])
            wide = jnp.concatenate([jnp.broadcast_to(four[j : j + 1], (8, 512)) for j in range(4)], axis=0)
            total_one = jnp.where(band_one == b, wide, total_one)
        m_two[a] = total_two.astype(BF16)
        m_one[a] = total_one.astype(BF16)

    settle(recv_sem, 0, (1, 2, 3), xr, yr, xyr, zr)
    build_planes(0, lambda x: inner[x], xr, yr, xyr)

    v_tiles = jnp.concatenate(
        [yr[0, 16:32], yr[1, 16:32]]
        + [xyr[corner(dx, dy), at : at + 16] for dx, at in ((-1, 0), (1, 16)) for dy in (-1, 1)],
        axis=0,
    )
    rims = nn(const("rim_rows")[:, 0:96], v_tiles)
    volp[120:128, :] = jnp.zeros((8, 768), F32)
    for p in range(6):
        mid = vol_rows(p - 1) if 1 <= p <= 4 else xr[p // 5, 128:160].astype(F32)
        plane = jnp.concatenate([mid, rims[p * 8 : p * 8 + 8]], axis=0)
        lanes = slice(p * 128, (p + 1) * 128)
        volp[40:80, lanes] = plane
        volp[0:40, lanes] = pltpu.roll(plane, 1, 1)
        volp[80:120, lanes] = pltpu.roll(plane, 127, 1)

    lane16 = lax.broadcasted_iota(jnp.int32, (16, 128), 1)
    slot = lax.shift_right_logical(lane16, 4)
    blocks = [jnp.zeros((16, 128), F32) for _ in range(4)]

    def add_taps(c):
        for a in range(3):
            g = nt(planes[c * 160 : c * 160 + 160, (2 - a) * 128 : (6 - a) * 128], acts[...])
            for b in range(3):
                t = (a * 3 + b) * 3 + c
                total = jnp.zeros((16, 128), F32)
                for y in range(8):
                    at = (y + 2 - b) * 16
                    total = jnp.where(slot == y, g[at : at + 16], total)
                for turn in (64, 32, 16):
                    total = total + pltpu.roll(total, turn, 1)
                blocks[t // 8] = jnp.where(slot == t % 8, total, blocks[t // 8])

    add_taps(1)
    settle(recv_sem, 0, (0,), xr, yr, xyr, zr)
    cols = close_planes(0, zr)

    back = nn(m_two[0], planes[:, 256:768]) + nn(m_two[1], planes[:, 128:640]) + nn(m_two[2], planes[:, 0:512])
    delta = jnp.where(acts[...].astype(F32) > 0, back, back * 0.3).astype(BF16)
    wide_delta = delta.astype(F32)
    bias_one = wide_delta[:, 0:128] + wide_delta[:, 128:256] + wide_delta[:, 256:384] + wide_delta[:, 384:512]

    def delta_at(x):
        return delta[:, x * 128 : (x + 1) * 128]

    rim_cols = nn(const("rim_cols"), cols.astype(BF16))
    lane40 = lax.broadcasted_iota(jnp.int32, (40, 128), 1)
    half8 = lax.broadcasted_iota(jnp.int32, (8, 1), 0) < 4
    for p in range(6):
        x = (p - 1) % 4
        dx = -1 if p == 0 else (1 if p == 5 else 0)
        lanes = slice(p * 128, (p + 1) * 128)
        r = {-1: 0, 1: 1, 0: 1}[dx]
        for tap, side, lane in ((0, 0, 0), (2, 1, 127)):
            k = 72 * side + 8 * way(dx, 0) + (3 if dx == 0 else r)
            low, high = (72 * side + 8 * way(dx, e) + r for e in (-1, 1))
            col = jnp.concatenate(
                [cols[j * 32 + x * 8 : j * 32 + x * 8 + 8, k : k + 1] for j in range(4)]
                + [
                    jnp.where(
                        half8,
                        rim_cols[p * 8 : p * 8 + 8, low : low + 1],
                        rim_cols[p * 8 : p * 8 + 8, high : high + 1],
                    )
                ],
                axis=0,
            )
            rows = slice(tap * 40, tap * 40 + 40)
            volp[rows, lanes] = jnp.where(lane40 == lane, jnp.broadcast_to(col, (40, 128)), volp[rows, lanes])

    y_of = const("y_of").astype(F32)
    sums = []
    for a in range(3):
        g = nt(delta, volp[:, a * 128 : (a + 4) * 128].astype(BF16))
        for b in range(3):
            total = jnp.zeros((16, 128), F32)
            for y in range(8):
                total = total + jnp.where(y_of == y + b, g[y * 16 : y * 16 + 16], 0.0)
            sums.append(total)
    sums = jnp.concatenate(sums, axis=1)
    top = sums.astype(BF16)
    rest = (sums - top.astype(F32)).astype(BF16)
    fold = fold_v[...]
    packed = nn(top, fold) + nn(rest, fold)

    def fold_y(v):
        out = v[0:16]
        for y in range(1, 8):
            out = out + v[y * 16 : y * 16 + 16]
        return jnp.broadcast_to(jnp.sum(out, axis=1, keepdims=True), (16, 128))

    share[64:80] = jnp.where(lane16 >= 108, fold_y(bias_one), packed)
    share[80:96] = jnp.zeros((16, 128), F32)

    add_taps(0)
    add_taps(2)
    blocks[3] = jnp.where(slot == 3, fold_y(bias_two), blocks[3])
    for k in range(4):
        share[k * 16 : k * 16 + 16] = blocks[k]

    for step in group_steps:
        t, where = in_group(step)
        pltpu.make_async_remote_copy(
            share.at[pl.ds(ROWS * t, ROWS)], got1.at[pl.ds(4 * group_at, ROWS)],
            red_send.at[0], red_recv.at[0], device_id=where, device_id_type=MESH,
        ).start()
    own = pltpu.make_async_copy(share.at[pl.ds(ROWS * group_at, ROWS)], got1.at[pl.ds(4 * group_at, ROWS)], own_sem.at[0])
    own.start()
    own.wait()

    xs2[0] = delta_at(0)
    xs2[1] = delta_at(3)
    for h in range(2):
        for at, x in ((0, 0), (1, 3), (2, 1), (3, 2)):
            ys2[h, at * 16 : at * 16 + 16] = delta_at(x)[112 * h : 112 * h + 16]
    z_face = nt(ends, jnp.concatenate([delta_at(x) for x in range(4)], axis=0))
    z_edge = nt(ends, edge_rows(delta_at))
    for f in range(2):
        face = [z_face[f : f + 1, x * 128 : (x + 1) * 128] for x in range(4)]
        zs2[f] = stack8([face[1], face[2], face[0], face[3], z_edge[f : f + 1]])
    exchange(1, xs2, xr2, ys2, yr2, xyr2, zs2, zr2)
    for x in range(4):
        inner[x] = delta_at(x)

    def await_rows(sem, ref, n):
        ref = ref.at[pl.ds(0, n * ROWS)]
        pltpu.make_async_copy(ref, ref, sem).wait()

    def total8(ref, n):
        out = ref[0:8]
        for i in range(1, n // 2):
            out = out + ref[i * 8 : i * 8 + 8]
        return out + pltpu.roll(out, 4, 0)

    await_rows(red_recv.at[0], got1, n_group - 1)
    mid1[...] = total8(got1, n_group)

    for d in line_steps:
        pltpu.make_async_remote_copy(
            mid1.at[pl.ds(0, ROWS)], got2.at[pl.ds(4 * line_at, ROWS)],
            red_send.at[1], red_recv.at[1], device_id=in_line(d), device_id_type=MESH,
        ).start()
    own = pltpu.make_async_copy(mid1.at[pl.ds(0, ROWS)], got2.at[pl.ds(4 * line_at, ROWS)], own_sem.at[1])
    own.start()
    own.wait()

    await_rows(red_recv.at[1], got2, n_line - 1)
    mid2[...] = total8(got2, n_line) * norm

    for step in group_steps:
        pltpu.make_async_remote_copy(
            mid2.at[pl.ds(0, ROWS)], summed.at[pl.ds(ROWS * group_at, ROWS)],
            red_send.at[2], red_recv.at[2], device_id=in_group(step)[1], device_id_type=MESH,
        ).start()
    own = pltpu.make_async_copy(mid2.at[pl.ds(0, ROWS)], summed.at[pl.ds(ROWS * group_at, ROWS)], own_sem.at[2])
    own.start()
    own.wait()
    settle(recv_sem, 1, range(4), xr2, yr2, xyr2, zr2)
    build_planes(1, lambda x: inner[x], xr2, yr2, xyr2)
    close_planes(1, zr2)
    grad = nn(m_one[0], planes[:, 256:768]) + nn(m_one[1], planes[:, 128:640]) + nn(m_one[2], planes[:, 0:512])
    for j in range(4):
        for x in range(4):
            gvol[j, x] = grad[j * 8 : j * 8 + 8, x * 128 : (x + 1) * 128]

    settle(send_sem, 0, range(4), xr, yr, xyr, zr)
    settle(send_sem, 1, range(4), xr2, yr2, xyr2, zr2)
    await_rows(red_send.at[0], got1, n_group - 1)
    await_rows(red_send.at[1], got2, n_line - 1)
    await_rows(red_recv.at[2], summed, n_group - 1)

    await_rows(red_send.at[2], summed, n_group - 1)


def finish(
    summed, gvol_v, gw1, gb1, gw2, gb2, gvol,
    gw1_v, gb1_v, gw2_v, gb2_v, sems,
):
    copies = [
        pltpu.make_async_copy(src, dst, sems.at[i])
        for i, (src, dst) in enumerate(((gvol_v, gvol), (gw2_v, gw2), (gw1_v, gw1), (gb1_v, gb1), (gb2_v, gb2)))
    ]
    copies[0].start()
    for k in range(4):
        block = summed[k * 16 : k * 16 + 16]
        for s in range(8):
            if k * 8 + s < 27:
                turned = pltpu.roll(block, (128 - 16 * s) % 128, 1) if s else block
                gw2_v[k * 8 + s] = turned[:, 0:16]
    copies[1].start()
    packed = summed[64:80].T
    for t in range(27):
        gw1_v[t] = packed[4 * t : 4 * t + 4, :]
    copies[2].start()
    gb1_v[...] = packed[108, :]
    gb2_v[...] = summed[48:64].T[48, :]
    copies[3].start()
    copies[4].start()
    for copy in copies:
        copy.wait()


def local(sizes, norm, volume, act_one, act_two, weight_one, weight_two, cotangent):
    narrow, wide, fold = constants()
    w1 = jnp.transpose(weight_one, (2, 3, 4, 1, 0)).reshape(27, CHAN_IN, CHAN)
    w2 = jnp.transpose(weight_two, (2, 3, 4, 0, 1)).reshape(27, CHAN, CHAN)
    n_group = sizes[0] * 4
    n_line = sizes[1] * (sizes[2] // 4)
    buf = lambda *shape: pltpu.VMEM(shape, BF16)
    buf32 = lambda *shape: pltpu.VMEM(shape, F32)
    block = (CHAN, NX, NY, NZ)
    summed, gvol = pl.pallas_call(
        functools.partial(kernel, sizes, norm),
        out_shape=(
            pltpu.VMEM((96, 128), F32),
            pltpu.VMEM((CHAN_IN, NX, NY, NZ), F32),
        ),
        in_specs=[pl.BlockSpec(memory_space=pl.ANY)] * 9,
        out_specs=tuple([pl.BlockSpec(memory_space=pltpu.VMEM)] * 2),
        scratch_shapes=[
            buf(CHAN_IN, NX, NY, NZ), buf(*block), buf(*block), buf(27, CHAN_IN, CHAN), buf(27, CHAN, CHAN), buf(*block),
            buf(NARROW, 128), buf(208, 512), buf(1152, 128),
            buf(2, 160, 128), buf(2, 160, 128), buf(2, 80, 128), buf(2, 80, 128), buf(4, 32, 128), buf32(2, 8, 128), buf32(2, 72, 128),
            buf(2, 128, 128), buf(2, 128, 128), buf(2, 64, 128), buf(2, 64, 128), buf(4, 16, 128), buf32(2, 8, 128), buf32(2, 72, 128),
            buf(4, 128, 128), buf(128, 512), buf(512, 768), buf32(2, 160, 768), buf32(128, 768), buf(3, 128, 512), buf(3, 32, 512),
            buf32(96, 128), buf32(4 * n_group, 128), buf32(4 * n_line, 128), buf32(8, 128), buf32(8, 128),
            pltpu.SemaphoreType.DMA((9,)), pltpu.SemaphoreType.DMA((3,)),
            pltpu.SemaphoreType.DMA((2, 4)), pltpu.SemaphoreType.DMA((2, 4)),
            pltpu.SemaphoreType.DMA((3,)), pltpu.SemaphoreType.DMA((3,)),
        ],
        compiler_params=pltpu.CompilerParams(collective_id=0, has_side_effects=True, vmem_limit_bytes=60 * 2**20),
        name="both_layers",
    )(volume, act_one, act_two, w1, w2, cotangent, narrow, wide, fold)
    shapes = ((27, CHAN_IN, CHAN), (CHAN,), (27, CHAN, CHAN), (CHAN,))
    gw1, gb1, gw2, gb2, gvol = pl.pallas_call(
        finish,
        out_shape=tuple(jax.ShapeDtypeStruct(shape, F32) for shape in shapes + ((CHAN_IN, NX, NY, NZ),)),
        in_specs=[pl.BlockSpec(memory_space=pltpu.VMEM)] * 2,
        out_specs=tuple([pl.BlockSpec(memory_space=pl.ANY)] * 5),
        scratch_shapes=[buf32(*shape) for shape in shapes] + [pltpu.SemaphoreType.DMA((5,))],
        compiler_params=pltpu.CompilerParams(vmem_limit_bytes=8 * 2**20),
        name="finish",
    )(summed, gvol)
    gw1 = jnp.transpose(gw1.reshape(3, 3, 3, CHAN_IN, CHAN), (4, 3, 0, 1, 2))
    gw2 = jnp.transpose(gw2.reshape(3, 3, 3, CHAN, CHAN), (3, 4, 0, 1, 2))
    return gw1, gb1, gw2, gb2, gvol


def solution(mesh):
    sizes = tuple(mesh.shape[name] for name in ("gx", "gy", "gz"))
    norm = 1.0 / math.sqrt(NX * NY * NZ * sizes[0] * sizes[1] * sizes[2])
    block = P(None, "gx", "gy", "gz")
    return jax.shard_map(
        functools.partial(local, sizes, norm),
        mesh=mesh,
        in_specs=(block, block, block, P(), P(), block),
        out_specs=(P(), P(), P(), P(), block),
        check_vma=False,
    )
```

```python
import functools
import math

import jax
import jax.numpy as jnp
import numpy as np
from jax import lax
from jax.experimental import pallas as pl
from jax.experimental.pallas import tpu as pltpu
from jax.sharding import PartitionSpec as P

CHAN_IN = 4
CHAN = 16
NX, NY, NZ = 4, 8, 128
F32, BF16 = jnp.float32, jnp.bfloat16
MESH = pl.DeviceIdType.MESH
ROWS = 3
SIDES = ((-1, 0), (1, 0), (0, -1), (0, 1), (-1, -1), (-1, 1), (1, -1), (1, 1))


def constants():
    r = np.arange(128)
    perm = np.zeros((128, 128), np.float32)
    perm[r, (r % 16) * 8 + r // 16] = 1
    eye = np.eye(128, dtype=np.float32)
    ends = np.zeros((16, 128), np.float32)
    ends[0, 0] = ends[1, 127] = 1
    tiles = np.zeros((32, 128), np.float32)
    for h in range(2):
        for x in range(4):
            for j in range(4):
                tiles[h * 16 + x * 4 + j, j * 32 + x * 8 + 7 * h] = 1
    rim_cols = np.zeros((48, 128), np.float32)
    rim_rows = np.zeros((48, 128), np.float32)
    for p in range(6):
        x = (p - 1) % 4
        for h in range(2):
            for j in range(4):
                rim_cols[p * 8 + h * 4 + j, j * 32 + x * 8 + 7 * (1 - h)] = 1
                tile = h if 1 <= p <= 4 else 2 + (0 if p == 0 else 2) + h
                rim_rows[p * 8 + h * 4 + j, tile * 16 + x * 4 + j] = 1
    spread = np.zeros((128, 128), np.float32)
    spread[r, r % 16] = 1
    narrow = np.concatenate([perm, eye, ends, tiles, rim_cols, rim_rows, spread])
    lane = np.arange(512)
    inside = lane < 480
    tap, end, chan = lane // 160, (lane % 160) // 16, lane % 16
    place = np.zeros((48, 512), np.float32)
    for c in range(3):
        for o in range(16):
            place[c * 16 + o] = inside & (tap == c) & (chan == o)
    y_two = (np.arange(128) // 16)[:, None]
    y_one = (np.arange(32) % 8)[:, None]
    band_two = np.where(inside[None], y_two + 2 - end[None], -9)
    band_one = np.where(inside[None], y_one + 2 - end[None], -9)
    wide = np.concatenate([place, band_two, band_one])
    rr = np.arange(128) % 40
    ok = np.arange(128) < 120
    row_y = np.where(rr < 32, 1 + rr % 8, np.where(rr < 36, 0, 9))
    row_j = np.where(rr < 32, rr // 8, rr % 4)
    row_c = np.arange(128) // 40
    y_of = np.broadcast_to(np.where(ok, row_y, -9)[None], (16, 128))
    fold = np.zeros((9, 128, 128), np.float32)
    for ab in range(9):
        for q in range(120):
            fold[ab, q, (ab * 3 + row_c[q]) * 4 + row_j[q]] = 1
    narrow = np.concatenate([narrow, y_of])
    return jnp.asarray(narrow, BF16), jnp.asarray(wide, BF16), jnp.asarray(fold.reshape(-1, 128), BF16)


AT = {}
_at = 0
for _name, _n in (("perm", 128), ("eye", 128), ("ends", 16), ("tiles", 32), ("rim_cols", 48), ("rim_rows", 48), ("spread", 128), ("y_of", 16)):
    AT[_name] = (_at, _n)
    _at += _n
NARROW = _at


def nt(a, b):
    return lax.dot_general(a, b, (((1,), (1,)), ((), ())), preferred_element_type=F32)


def nn(a, b):
    return jnp.dot(a, b, preferred_element_type=F32)


def way(dx, dy):
    return (dx + 1) * 3 + dy + 1


def corner(dx, dy):
    return (dx + 1) + (dy + 1) // 2


def kernel(
    sizes, norm,
    vol_h, act1_h, act2_h, w1_h, w2_h, cot_h, narrow_h, wide_h, fold_h,
    summed, gvol,
    vol_v, act1_v, act2_v, w1_v, w2_v, cot_v, narrow_v, wide_v, fold_v,
    xs, xr, ys, yr, xyr, zs, zr,
    xs2, xr2, ys2, yr2, xyr2, zs2, zr2,
    inner, acts, planes, rotated, volp, m_two, m_one, share, got1, got2, mid1, mid2,
    load_sem, own_sem, send_sem, recv_sem, red_send, red_recv,
):
    n_gx, n_gy, n_gz = sizes
    n_y = 4
    n_hi = n_gz // n_y
    n_group = n_gx * n_y
    n_line = n_gy * n_hi
    gx, gy, gz = lax.axis_index("gx"), lax.axis_index("gy"), lax.axis_index("gz")
    y_pos, hi_pos = lax.rem(gz, n_y), lax.div(gz, n_y)
    group_at = gx * n_y + y_pos
    line_at = hi_pos * n_gy + gy

    loads = [
        pltpu.make_async_copy(src, dst, load_sem.at[i])
        for i, (src, dst) in enumerate(
            ((cot_h, cot_v), (act2_h, act2_v), (narrow_h, narrow_v), (vol_h, vol_v), (act1_h, act1_v), (wide_h, wide_v), (w2_h, w2_v), (w1_h, w1_v), (fold_h, fold_v))
        )
    ]
    for copy in loads[:4]:
        copy.start()

    gx_at = [lax.rem(gx + d, n_gx) for d in range(n_gx)]
    gy_at = [lax.rem(gy + d, n_gy) for d in range(n_gy)]
    gz_at = [lax.rem(gz + d, n_gz) for d in range(n_gz)]
    y_at = [lax.rem(y_pos + d, n_y) for d in range(n_y)]
    line_to = [lax.rem(line_at + d, n_line) for d in range(n_line)]
    run_base = hi_pos * n_y

    def near(dx, dy, dz):
        return gx_at[dx], gy_at[dy], gz_at[dz]

    def ring(d, n):
        return min(d, n - d)

    group_steps = sorted(
        ((d, e) for d in range(n_gx) for e in range(n_y) if (d, e) != (0, 0)),
        key=lambda p: -(ring(p[0], n_gx) / 2 + ring(p[1], n_y)),
    )
    line_steps = sorted(range(1, n_line), key=lambda d: -ring(d, n_line))

    def in_group(step):
        d, e = step
        return gx_at[d] * n_y + y_at[e], (gx_at[d], gy, run_base + y_at[e])

    def in_line(d):
        return gx, lax.rem(line_to[d], n_gy), lax.div(line_to[d], n_gy) * n_y + y_pos

    barrier = pltpu.get_barrier_semaphore()
    for dz in (-1, 1):
        for dx in (-1, 0, 1):
            for dy in (-1, 0, 1):
                if (dx, dy, dz) != (0, 0, 0):
                    pl.semaphore_signal(barrier, inc=1, device_id=near(dx, dy, dz), device_id_type=MESH)

    for d in line_steps:
        pl.semaphore_signal(barrier, inc=1, device_id=in_line(d), device_id_type=MESH)
    for dz in (0,):
        for dx in (-1, 0, 1):
            for dy in (-1, 0, 1):
                if (dx, dy, dz) != (0, 0, 0):
                    pl.semaphore_signal(barrier, inc=1, device_id=near(dx, dy, dz), device_id_type=MESH)

    for step in group_steps:
        pl.semaphore_signal(barrier, inc=1, device_id=in_group(step)[1], device_id_type=MESH)
    for copy in loads[4:]:
        copy.start()

    def const(name):
        at, n = AT[name]
        return narrow_v[at : at + n, :]

    for i in range(4):
        loads[i].wait()
    perm, eye, ends = const("perm"), const("eye"), const("ends")

    def rows_of(ref, x):
        return ref[:, x].astype(F32).reshape(128, 128)

    def edge_rows(inner_at):
        return jnp.concatenate(
            [inner_at(x)[0:16] for x in range(4)] + [inner_at(x)[112:128] for x in range(4)], axis=0
        )

    row8 = lax.broadcasted_iota(jnp.int32, (8, 128), 0)

    def stack8(rows):
        out = jnp.zeros((8, 128), F32)
        for i, row in enumerate(rows):
            out = jnp.where(row8 == i, jnp.broadcast_to(row, (8, 128)), out)
        return out

    deltas = []
    for x in range(4):
        v = rows_of(cot_v, x)
        deltas.append(jnp.where(rows_of(act2_v, x) > 0, v, v * 0.3).astype(BF16))
    turned = nn(perm, jnp.concatenate(deltas, axis=1))
    bias_two = turned[:, 0:128] + turned[:, 128:256] + turned[:, 256:384] + turned[:, 384:512]
    turned = turned.astype(BF16)
    for x in range(4):
        inner[x] = turned[:, x * 128 : (x + 1) * 128]
    volflat = vol_v[...].astype(F32).reshape(128, 128).astype(BF16)
    vol_tiles = nn(const("tiles"), volflat).astype(BF16)

    def vol_rows(x):
        return vol_v[:, x].astype(F32).reshape(32, 128)

    xs[0, 0:128] = inner[0]
    xs[1, 0:128] = inner[3]
    xs[0, 128:160] = vol_rows(0).astype(BF16)
    xs[1, 128:160] = vol_rows(3).astype(BF16)
    for h in range(2):
        for at, x in ((0, 0), (2, 3), (3, 1), (4, 2)):
            ys[h, at * 16 : at * 16 + 16] = inner[x][112 * h : 112 * h + 16]
        ys[h, 16:32] = vol_tiles[16 * h : 16 * h + 16]
    z_face = nt(ends, jnp.concatenate([inner[x] for x in range(4)], axis=0))
    z_edge = nt(ends, edge_rows(lambda x: inner[x]))
    z_vol = nt(ends, volflat)
    for f in range(2):
        face = [z_face[f : f + 1, x * 128 : (x + 1) * 128] for x in range(4)]
        edge, flat = z_edge[f : f + 1], z_vol[f : f + 1]
        zs[f] = stack8([face[1], face[2], face[0], flat, face[3], edge, flat])

    pl.semaphore_wait(barrier, 26 + (n_line - 1) + (n_group - 1))

    def exchange(phase, xs, xr, ys, yr, xyr, zs, zr):
        first = phase == 0
        out = []

        def send(kind, src, dst, where):
            copy = pltpu.make_async_remote_copy(
                src, dst, send_sem.at[phase, kind], recv_sem.at[phase, kind], device_id=where, device_id_type=MESH
            )
            copy.start()
            out.append(copy)

        for dz in (-1, 1):
            f, side = (1 if dz == 1 else 0), (0 if dz == 1 else 1)
            for dx in (-1, 0, 1):
                for dy in (-1, 0, 1):
                    if first:
                        at, n = {-1: (2, 2), 1: (3, 2), 0: (0, 5) if dy == 0 else (5, 2)}[dx]
                    else:
                        at, n = {-1: (2, 1), 1: (3, 1), 0: (0, 4) if dy == 0 else (4, 1)}[dx]
                    send(0, zs.at[f, pl.ds(at, n)], zr.at[side, pl.ds(8 * way(-dx, -dy), n)], near(dx, dy, dz))
        for dx in (-1, 1):
            send(1, xs.at[(dx + 1) // 2], xr.at[(1 - dx) // 2], near(dx, 0, 0))
        for dy in (-1, 1):
            send(2, ys.at[(dy + 1) // 2], yr.at[(1 - dy) // 2], near(0, dy, 0))
        for dx in (-1, 1):
            for dy in (-1, 1):
                if first:
                    at, n = (0 if dx == -1 else 16), 32
                else:
                    at, n = (0 if dx == -1 else 16), 16
                send(3, ys.at[(dy + 1) // 2, pl.ds(at, n)], xyr.at[corner(-dx, -dy)], near(dx, dy, 0))

    def settle(sems, phase, kinds, xr, yr, xyr, zr):
        refs = (zr.at[0, pl.ds(0, 42 if phase == 0 else 24)], xr, yr, xyr)
        for kind in kinds:
            pltpu.make_async_copy(refs[kind], refs[kind], sems.at[phase, kind]).wait()

    lane_of = lax.broadcasted_iota(jnp.int32, (160, 128), 1)

    TURNS = ((0, 1, 127, 127), (2, 0, 1, 0))

    def build_planes(phase, inner_at, xr, yr, xyr):
        first = phase == 0
        tile_at = {0: 0, 3: 2, 1: 3, 2: 4} if first else {0: 0, 3: 1, 1: 2, 2: 3}
        for p in range(6):
            if 1 <= p <= 4:
                x = p - 1
                low = yr[0, tile_at[x] * 16 : tile_at[x] * 16 + 16]
                mid = inner_at(x)
                high = yr[1, tile_at[x] * 16 : tile_at[x] * 16 + 16]
            else:
                dx = -1 if p == 0 else 1
                at = (16 if dx == -1 else 0) if first else 0
                low = xyr[corner(dx, -1), at : at + 16]
                mid = xr[(dx + 1) // 2, 0:128]
                high = xyr[corner(dx, 1), at : at + 16]
            plane = jnp.concatenate([low, mid, high], axis=0)
            lanes = slice(p * 128, (p + 1) * 128)
            planes[160:320, lanes] = plane
            plane = plane.astype(F32)
            for tap, side, turn, lane in TURNS:
                rotated[side, :, lanes] = pltpu.roll(plane, turn, 1)

    def close_planes(phase, zr):
        first = phase == 0
        cols = nt(eye, zr[...].reshape(144, 128).astype(BF16))
        face_at = {0: 2, 3: 4, 1: 0, 2: 1} if first else {0: 2, 3: 3, 1: 0, 2: 1}
        for p in range(6):
            if 1 <= p <= 4:
                x = p - 1
                pick = (
                    (64 + 16 * x, 80 + 16 * x, 8 * way(0, -1)),
                    (0, 128, 8 * way(0, 0) + face_at[x]),
                    (16 * x, 16 * x + 16, 8 * way(0, 1)),
                )
            else:
                dx = -1 if p == 0 else 1
                r = (1 if dx == -1 else 0) if first else 0
                pick = (
                    (112, 128, 8 * way(dx, -1) + r),
                    (0, 128, 8 * way(dx, 0) + r),
                    (0, 16, 8 * way(dx, 1) + r),
                )
            lanes = slice(p * 128, (p + 1) * 128)
            for tap, side, turn, lane in TURNS:
                col = jnp.concatenate(
                    [cols[a:b, 72 * side + k : 72 * side + k + 1] for a, b, k in pick], axis=0
                )
                shifted = jnp.where(lane_of == lane, jnp.broadcast_to(col, (160, 128)), rotated[side, :, lanes])
                planes[tap * 160 : tap * 160 + 160, lanes] = shifted.astype(BF16)
        return cols

    exchange(0, xs, xr, ys, yr, xyr, zs, zr)

    for i in range(4, 9):
        loads[i].wait()
    turned = nn(perm, jnp.concatenate([rows_of(act1_v, x).astype(BF16) for x in range(4)], axis=1))
    acts[...] = turned.astype(BF16)
    planes[480:512, :] = jnp.zeros((32, 768), BF16)
    place = wide_v[0:48, :]
    band_two = wide_v[48:176, :].astype(F32)
    band_one = wide_v[176:208, :].astype(F32)
    spread = const("spread")[:, 0:16]
    for a in range(3):
        total_two = jnp.zeros((128, 512), F32)
        total_one = jnp.zeros((32, 512), F32)
        for b in range(3):
            t = (a * 3 + b) * 3
            group = w2_v[t : t + 3].reshape(48, 16)
            wide = nn(nt(spread, group).astype(BF16), place)
            total_two = jnp.where(band_two == b, wide, total_two)
            four = jnp.zeros((4, 512), F32)
            for c in range(3):
                four = four + nn(w1_v[t + c], place[c * 16 : c * 16 + 16])
            wide = jnp.concatenate([jnp.broadcast_to(four[j : j + 1], (8, 512)) for j in range(4)], axis=0)
            total_one = jnp.where(band_one == b, wide, total_one)
        m_two[a] = total_two.astype(BF16)
        m_one[a] = total_one.astype(BF16)

    settle(recv_sem, 0, (1, 2, 3), xr, yr, xyr, zr)
    build_planes(0, lambda x: inner[x], xr, yr, xyr)

    v_tiles = jnp.concatenate(
        [yr[0, 16:32], yr[1, 16:32]]
        + [xyr[corner(dx, dy), at : at + 16] for dx, at in ((-1, 0), (1, 16)) for dy in (-1, 1)],
        axis=0,
    )
    rims = nn(const("rim_rows")[:, 0:96], v_tiles)
    volp[120:128, :] = jnp.zeros((8, 768), F32)
    for p in range(6):
        mid = vol_rows(p - 1) if 1 <= p <= 4 else xr[p // 5, 128:160].astype(F32)
        plane = jnp.concatenate([mid, rims[p * 8 : p * 8 + 8]], axis=0)
        lanes = slice(p * 128, (p + 1) * 128)
        volp[40:80, lanes] = plane
        volp[0:40, lanes] = pltpu.roll(plane, 1, 1)
        volp[80:120, lanes] = pltpu.roll(plane, 127, 1)

    lane16 = lax.broadcasted_iota(jnp.int32, (16, 128), 1)
    slot = lax.shift_right_logical(lane16, 4)
    blocks = [jnp.zeros((16, 128), F32) for _ in range(4)]

    def add_taps(c):
        for a in range(3):
            g = nt(planes[c * 160 : c * 160 + 160, (2 - a) * 128 : (6 - a) * 128], acts[...])
            for b in range(3):
                t = (a * 3 + b) * 3 + c
                total = jnp.zeros((16, 128), F32)
                for y in range(8):
                    at = (y + 2 - b) * 16
                    total = jnp.where(slot == y, g[at : at + 16], total)
                for turn in (64, 32, 16):
                    total = total + pltpu.roll(total, turn, 1)
                blocks[t // 8] = jnp.where(slot == t % 8, total, blocks[t // 8])

    add_taps(1)
    settle(recv_sem, 0, (0,), xr, yr, xyr, zr)
    cols = close_planes(0, zr)

    back = nn(m_two[0], planes[:, 256:768]) + nn(m_two[1], planes[:, 128:640]) + nn(m_two[2], planes[:, 0:512])
    delta = jnp.where(acts[...].astype(F32) > 0, back, back * 0.3).astype(BF16)
    wide_delta = delta.astype(F32)
    bias_one = wide_delta[:, 0:128] + wide_delta[:, 128:256] + wide_delta[:, 256:384] + wide_delta[:, 384:512]

    def delta_at(x):
        return delta[:, x * 128 : (x + 1) * 128]

    rim_cols = nn(const("rim_cols"), cols.astype(BF16))
    lane40 = lax.broadcasted_iota(jnp.int32, (40, 128), 1)
    half8 = lax.broadcasted_iota(jnp.int32, (8, 1), 0) < 4
    for p in range(6):
        x = (p - 1) % 4
        dx = -1 if p == 0 else (1 if p == 5 else 0)
        lanes = slice(p * 128, (p + 1) * 128)
        r = {-1: 0, 1: 1, 0: 1}[dx]
        for tap, side, lane in ((0, 0, 0), (2, 1, 127)):
            k = 72 * side + 8 * way(dx, 0) + (3 if dx == 0 else r)
            low, high = (72 * side + 8 * way(dx, e) + r for e in (-1, 1))
            col = jnp.concatenate(
                [cols[j * 32 + x * 8 : j * 32 + x * 8 + 8, k : k + 1] for j in range(4)]
                + [
                    jnp.where(
                        half8,
                        rim_cols[p * 8 : p * 8 + 8, low : low + 1],
                        rim_cols[p * 8 : p * 8 + 8, high : high + 1],
                    )
                ],
                axis=0,
            )
            rows = slice(tap * 40, tap * 40 + 40)
            volp[rows, lanes] = jnp.where(lane40 == lane, jnp.broadcast_to(col, (40, 128)), volp[rows, lanes])

    y_of = const("y_of").astype(F32)
    sums = []
    for a in range(3):
        g = nt(delta, volp[:, a * 128 : (a + 4) * 128].astype(BF16))
        for b in range(3):
            total = jnp.zeros((16, 128), F32)
            for y in range(8):
                total = total + jnp.where(y_of == y + b, g[y * 16 : y * 16 + 16], 0.0)
            sums.append(total)
    sums = jnp.concatenate(sums, axis=1)
    top = sums.astype(BF16)
    rest = (sums - top.astype(F32)).astype(BF16)
    fold = fold_v[...]
    packed = nn(top, fold) + nn(rest, fold)

    def fold_y(v):
        out = v[0:16]
        for y in range(1, 8):
            out = out + v[y * 16 : y * 16 + 16]
        return jnp.broadcast_to(jnp.sum(out, axis=1, keepdims=True), (16, 128))

    share[64:80] = jnp.where(lane16 >= 108, fold_y(bias_one), packed)
    share[80:96] = jnp.zeros((16, 128), F32)

    add_taps(0)
    add_taps(2)
    blocks[3] = jnp.where(slot == 3, fold_y(bias_two), blocks[3])
    for k in range(4):
        share[k * 16 : k * 16 + 16] = blocks[k]

    for step in group_steps:
        t, where = in_group(step)
        pltpu.make_async_remote_copy(
            share.at[pl.ds(ROWS * t, ROWS)], got1.at[pl.ds(4 * group_at, ROWS)],
            red_send.at[0], red_recv.at[0], device_id=where, device_id_type=MESH,
        ).start()
    own = pltpu.make_async_copy(share.at[pl.ds(ROWS * group_at, ROWS)], got1.at[pl.ds(4 * group_at, ROWS)], own_sem.at[0])
    own.start()
    own.wait()

    xs2[0] = delta_at(0)
    xs2[1] = delta_at(3)
    for h in range(2):
        for at, x in ((0, 0), (1, 3), (2, 1), (3, 2)):
            ys2[h, at * 16 : at * 16 + 16] = delta_at(x)[112 * h : 112 * h + 16]
    z_face = nt(ends, jnp.concatenate([delta_at(x) for x in range(4)], axis=0))
    z_edge = nt(ends, edge_rows(delta_at))
    for f in range(2):
        face = [z_face[f : f + 1, x * 128 : (x + 1) * 128] for x in range(4)]
        zs2[f] = stack8([face[1], face[2], face[0], face[3], z_edge[f : f + 1]])
    exchange(1, xs2, xr2, ys2, yr2, xyr2, zs2, zr2)
    for x in range(4):
        inner[x] = delta_at(x)

    def await_rows(sem, ref, n):
        ref = ref.at[pl.ds(0, n * ROWS)]
        pltpu.make_async_copy(ref, ref, sem).wait()

    def total8(ref, n):
        out = ref[0:8]
        for i in range(1, n // 2):
            out = out + ref[i * 8 : i * 8 + 8]
        return out + pltpu.roll(out, 4, 0)

    await_rows(red_recv.at[0], got1, n_group - 1)
    mid1[...] = total8(got1, n_group)

    for d in line_steps:
        pltpu.make_async_remote_copy(
            mid1.at[pl.ds(0, ROWS)], got2.at[pl.ds(4 * line_at, ROWS)],
            red_send.at[1], red_recv.at[1], device_id=in_line(d), device_id_type=MESH,
        ).start()
    own = pltpu.make_async_copy(mid1.at[pl.ds(0, ROWS)], got2.at[pl.ds(4 * line_at, ROWS)], own_sem.at[1])
    own.start()
    own.wait()

    await_rows(red_recv.at[1], got2, n_line - 1)
    mid2[...] = total8(got2, n_line) * norm

    for step in group_steps:
        pltpu.make_async_remote_copy(
            mid2.at[pl.ds(0, ROWS)], summed.at[pl.ds(ROWS * group_at, ROWS)],
            red_send.at[2], red_recv.at[2], device_id=in_group(step)[1], device_id_type=MESH,
        ).start()
    own = pltpu.make_async_copy(mid2.at[pl.ds(0, ROWS)], summed.at[pl.ds(ROWS * group_at, ROWS)], own_sem.at[2])
    own.start()
    own.wait()
    settle(recv_sem, 1, range(4), xr2, yr2, xyr2, zr2)
    build_planes(1, lambda x: inner[x], xr2, yr2, xyr2)
    close_planes(1, zr2)
    grad = nn(m_one[0], planes[:, 256:768]) + nn(m_one[1], planes[:, 128:640]) + nn(m_one[2], planes[:, 0:512])
    for j in range(4):
        for x in range(4):
            gvol[j, x] = grad[j * 8 : j * 8 + 8, x * 128 : (x + 1) * 128]

    settle(send_sem, 0, range(4), xr, yr, xyr, zr)
    settle(send_sem, 1, range(4), xr2, yr2, xyr2, zr2)
    await_rows(red_send.at[0], got1, n_group - 1)
    await_rows(red_send.at[1], got2, n_line - 1)
    await_rows(red_recv.at[2], summed, n_group - 1)

    await_rows(red_send.at[2], summed, n_group - 1)


def finish(
    summed, gvol_v, gw1, gb1, gw2, gb2, gvol,
    gw1_v, gb1_v, gw2_v, gb2_v, sems,
):
    copies = [
        pltpu.make_async_copy(src, dst, sems.at[i])
        for i, (src, dst) in enumerate(((gvol_v, gvol), (gw2_v, gw2), (gw1_v, gw1), (gb1_v, gb1), (gb2_v, gb2)))
    ]
    copies[0].start()
    for k in range(4):
        block = summed[k * 16 : k * 16 + 16]
        for s in range(8):
            if k * 8 + s < 27:
                turned = pltpu.roll(block, (128 - 16 * s) % 128, 1) if s else block
                gw2_v[k * 8 + s] = turned[:, 0:16]
    copies[1].start()
    packed = summed[64:80].T
    for t in range(27):
        gw1_v[t] = packed[4 * t : 4 * t + 4, :]
    copies[2].start()
    gb1_v[...] = packed[108, :]
    gb2_v[...] = summed[48:64].T[48, :]
    copies[3].start()
    copies[4].start()
    for copy in copies:
        copy.wait()


def local(sizes, norm, volume, act_one, act_two, weight_one, weight_two, cotangent):
    narrow, wide, fold = constants()
    w1 = jnp.transpose(weight_one, (2, 3, 4, 1, 0)).reshape(27, CHAN_IN, CHAN)
    w2 = jnp.transpose(weight_two, (2, 3, 4, 0, 1)).reshape(27, CHAN, CHAN)
    n_group = sizes[0] * 4
    n_line = sizes[1] * (sizes[2] // 4)
    buf = lambda *shape: pltpu.VMEM(shape, BF16)
    buf32 = lambda *shape: pltpu.VMEM(shape, F32)
    block = (CHAN, NX, NY, NZ)
    summed, gvol = pl.pallas_call(
        functools.partial(kernel, sizes, norm),
        out_shape=(
            pltpu.VMEM((96, 128), F32),
            pltpu.VMEM((CHAN_IN, NX, NY, NZ), F32),
        ),
        in_specs=[pl.BlockSpec(memory_space=pl.ANY)] * 9,
        out_specs=tuple([pl.BlockSpec(memory_space=pltpu.VMEM)] * 2),
        scratch_shapes=[
            buf(CHAN_IN, NX, NY, NZ), buf(*block), buf(*block), buf(27, CHAN_IN, CHAN), buf(27, CHAN, CHAN), buf(*block),
            buf(NARROW, 128), buf(208, 512), buf(1152, 128),
            buf(2, 160, 128), buf(2, 160, 128), buf(2, 80, 128), buf(2, 80, 128), buf(4, 32, 128), buf32(2, 8, 128), buf32(2, 72, 128),
            buf(2, 128, 128), buf(2, 128, 128), buf(2, 64, 128), buf(2, 64, 128), buf(4, 16, 128), buf32(2, 8, 128), buf32(2, 72, 128),
            buf(4, 128, 128), buf(128, 512), buf(512, 768), buf32(2, 160, 768), buf32(128, 768), buf(3, 128, 512), buf(3, 32, 512),
            buf32(96, 128), buf32(4 * n_group, 128), buf32(4 * n_line, 128), buf32(8, 128), buf32(8, 128),
            pltpu.SemaphoreType.DMA((9,)), pltpu.SemaphoreType.DMA((3,)),
            pltpu.SemaphoreType.DMA((2, 4)), pltpu.SemaphoreType.DMA((2, 4)),
            pltpu.SemaphoreType.DMA((3,)), pltpu.SemaphoreType.DMA((3,)),
        ],
        compiler_params=pltpu.CompilerParams(collective_id=0, has_side_effects=True, vmem_limit_bytes=60 * 2**20),
        name="both_layers",
    )(volume, act_one, act_two, w1, w2, cotangent, narrow, wide, fold)
    shapes = ((27, CHAN_IN, CHAN), (CHAN,), (27, CHAN, CHAN), (CHAN,))
    gw1, gb1, gw2, gb2, gvol = pl.pallas_call(
        finish,
        out_shape=tuple(jax.ShapeDtypeStruct(shape, F32) for shape in shapes + ((CHAN_IN, NX, NY, NZ),)),
        in_specs=[pl.BlockSpec(memory_space=pltpu.VMEM)] * 2,
        out_specs=tuple([pl.BlockSpec(memory_space=pl.ANY)] * 5),
        scratch_shapes=[buf32(*shape) for shape in shapes] + [pltpu.SemaphoreType.DMA((5,))],
        compiler_params=pltpu.CompilerParams(vmem_limit_bytes=8 * 2**20),
        name="finish",
    )(summed, gvol)
    gw1 = jnp.transpose(gw1.reshape(3, 3, 3, CHAN_IN, CHAN), (4, 3, 0, 1, 2))
    gw2 = jnp.transpose(gw2.reshape(3, 3, 3, CHAN, CHAN), (3, 4, 0, 1, 2))
    return gw1, gb1, gw2, gb2, gvol


def solution(mesh):
    sizes = tuple(mesh.shape[name] for name in ("gx", "gy", "gz"))
    norm = 1.0 / math.sqrt(NX * NY * NZ * sizes[0] * sizes[1] * sizes[2])
    block = P(None, "gx", "gy", "gz")
    return jax.shard_map(
        functools.partial(local, sizes, norm),
        mesh=mesh,
        in_specs=(block, block, block, P(), P(), block),
        out_specs=(P(), P(), P(), P(), block),
        check_vma=False,
    )
```
